32 devices in a mesh: replica: 2 (over x), tp: 8 (over z, y), sub: 2 (over core).
Axes of the slice: x: 2, y: 2, z: 4, core: 2. Of those that a mesh axis runs over, the one named last changes fastest.
Arguments:
- hidden_in: bfloat16 [8, 8192], P('replica'), parts along dimension 0, may hold values from -6 to 6
- norm_gain: float32 [16384], P('replica'), parts along dimension 0, may hold values from 0.1 to 1.9
- wqkv_old: bfloat16 [16, 2, 1280, 4096], P(('replica', 'tp'), 'sub'), parts along dimension 0, may hold values from -0.1875 to 0.1875
- wo: bfloat16 [16384, 8192], P(('replica', 'tp', 'sub')), parts along dimension 0, may hold values from -0.0625 to 0.0625
- key_cache: bfloat16 [8, 4096, 1024], P('replica', ('tp', 'sub')), parts along dimension 0, may hold values from -240 to 240
- value_cache: bfloat16 [8, 4096, 1024], P('replica', ('tp', 'sub')), parts along dimension 0, may hold values from -6 to 6
- lengths: int32 [8], P('replica'), parts along dimension 0, may hold values from 1 to 4096
- section_order: int32 [32], P('replica'), parts along dimension 0, may hold values from 0 to 15, each once
Outputs:
- mixed_out: bfloat16 [8, 8192], P('replica'), parts along dimension 0
- wqkv_new: bfloat16 [16, 2, 640, 8192], P(('replica', 'tp'), 'sub'), parts along dimension 0
The draws below stay inside these ranges and needn't reach their ends.
There are 2 independent parts, one for each index of `replica`. The reference program is written for one: setup_inputs(seed, part) draws one part's arguments, and reference() takes and returns one part's arrays. A program takes and returns all parts, laid end to end along the dimension named above; each array names one. Nothing has to cross between parts.
Inputs may be any that keep to these rules, and one draw needn't show every extreme that they name: `section_order`: each input row block appears once. The new token's position is lengths[b].
All inputs are finite; a program needn't handle non-finite values.
Results may differ from the reference program's by a relative error of at most 0.0085.
The reference program's roundings to bfloat16 on the way (of `full_t`, `normed`, `projected` and `attended`) count: a program that leaves them out, or rounds other values in their place, can miss the bound.
Values may be sent and summed in bfloat16 or wider, within the bound.
A program may use at most 128 MiB of HBM per device.

```python
import math
import jax
import jax.numpy as jnp
from jax import lax

D = 8192
HEADS = 64
KV_HEADS = 8
HEAD_DIM = 128
RANKS = 8
ROW_BLOCKS = 16
SEQS = 4
CACHE_LEN = 4096
QKV = 10240
RANK_COLS = 1280
COLS_DEV = 640
ROWS_OLD = 4096
BLOCK_ROWS = 512
N_TP = 8


def draw_key_cache(key, part):
    base = jax.random.normal(jax.random.fold_in(key, 11), (SEQS, CACHE_LEN, KV_HEADS * HEAD_DIM), jnp.float32)
    return jnp.clip(base, -6.0, 6.0).astype(jnp.bfloat16)


def place_ends(entries, key, smallest, top_value):
    spot = [jax.random.randint(jax.random.fold_in(key, axis), (), 0, length) for axis, length in enumerate(entries.shape)]
    widest = entries.shape.index(max(entries.shape))
    neighbour = spot[:widest] + [(spot[widest] + 1) % entries.shape[widest]] + spot[widest + 1:]
    return entries.at[tuple(spot)].set(smallest).at[tuple(neighbour)].set(top_value)


def level_of(key, extent, split, smallest, high):
    gain = 1.0
    for dim, shards_of in split:
        steps = jax.random.uniform(jax.random.fold_in(jax.random.fold_in(key, 6), dim), (shards_of,), jnp.float32, smallest / len(split), high / len(split))
        gain = gain * jnp.repeat(jnp.exp(steps), extent[dim] // shards_of).reshape((-1,) + (1,) * (len(extent) - 1 - dim))
    return gain


def normal_values(own_key, shape, scale, limit, pieces=(), kind=jnp.bfloat16):
    array = scale * jax.random.normal(own_key, shape, jnp.float32)
    if pieces:
        array = array * level_of(own_key, shape, pieces, -0.22, 0.18)
    return jnp.clip(array, -limit, limit).astype(kind)


def setup_inputs(seed: int = 0, part: int = 0) -> dict:
    seeds = jax.random.split(jax.random.key(seed), 9)
    part_keys = jax.random.split(jax.random.fold_in(seeds[8], part), 9)
    return {
        "hidden_in": normal_values(part_keys[0], (SEQS, D), 1.0, 6.0),
        "norm_gain": jnp.clip(1.0 + 0.18 * jax.random.normal(part_keys[1], (D,), jnp.float32), 0.1, 1.9),
        "wqkv_old": normal_values(part_keys[2], (N_TP, 2, RANK_COLS, ROWS_OLD), (D // 9) ** -0.5, 0.1875, ((0, 8), (1, 2))),
        "wo": normal_values(part_keys[3], (HEADS * HEAD_DIM, D), (HEADS * HEAD_DIM) ** -0.5, 0.0625, ((0, 16),)),
        "key_cache": draw_key_cache(jax.random.fold_in(jax.random.fold_in(seeds[8], part), 71), part),
        "value_cache": normal_values(part_keys[5], (SEQS, CACHE_LEN, KV_HEADS * HEAD_DIM), 1.0, 6.0, ((1, 16),)),
        "lengths": place_ends(jax.random.randint(part_keys[6], (SEQS,), 1, CACHE_LEN + 1), jax.random.fold_in(part_keys[6], 1), 1, CACHE_LEN).astype(jnp.int32),
        "section_order": jax.random.permutation(part_keys[7], ROW_BLOCKS).astype(jnp.int32),
    }


def rotary(values, positions):
    half = values.shape[-1] // 2
    freqs = 500000.0 ** (-jnp.arange(half, dtype=jnp.float32) * 2.0 / values.shape[-1])
    angles = positions.astype(jnp.float32)[:, None] * freqs[None, :]
    cosine = jnp.cos(angles)[:, None, :]
    sine = jnp.sin(angles)[:, None, :]
    first_half = values[..., :half]
    second_half = values[..., half:]
    return jnp.concatenate([first_half * cosine - second_half * sine, second_half * cosine + first_half * sine], -1)

def rms_normed(hidden_in, norm_gain):
    widened = hidden_in.astype(jnp.float32)
    factor = lax.rsqrt(lax.optimization_barrier(jnp.mean(widened * widened, -1, keepdims=True)) + 1e-05)
    return (widened, (widened * factor * norm_gain).astype(jnp.bfloat16))

def reference(hidden_in, norm_gain, wqkv_old, wo, key_cache, value_cache, lengths, section_order):
    section_count = N_TP // 4
    per_section = ROW_BLOCKS // section_count
    groups = HEADS // KV_HEADS
    q_width = HEADS * HEAD_DIM
    kv_width = KV_HEADS * HEAD_DIM
    by_rank = wqkv_old.reshape(section_count, RANKS, RANK_COLS, per_section, BLOCK_ROWS)
    blocks = jnp.transpose(by_rank, (0, 3, 1, 2, 4)).reshape(ROW_BLOCKS, RANKS, RANK_COLS, BLOCK_ROWS)
    ordered = jnp.zeros_like(blocks).at[section_order].set(blocks)
    full_t = jnp.transpose(ordered, (1, 2, 0, 3)).reshape(QKV, D)
    wqkv_new = jnp.transpose(full_t.reshape(4, 2, section_count, COLS_DEV, D), (2, 0, 1, 3, 4)).reshape(N_TP, 2, COLS_DEV, D)
    widened, normed = rms_normed(hidden_in, norm_gain)
    projected = lax.dot_general(normed, full_t, (((1,), (1,)), ((), ())), preferred_element_type=jnp.float32).astype(jnp.bfloat16)
    queries = rotary(projected[:, :q_width].astype(jnp.float32).reshape(SEQS, HEADS, HEAD_DIM), lengths).astype(jnp.bfloat16)
    new_keys = rotary(projected[:, q_width:q_width + kv_width].astype(jnp.float32).reshape(SEQS, KV_HEADS, HEAD_DIM), lengths).astype(jnp.bfloat16)
    new_values = projected[:, q_width + kv_width:].astype(jnp.float32).reshape(SEQS, KV_HEADS, HEAD_DIM)
    grouped = queries.astype(jnp.float32).reshape(SEQS, KV_HEADS, groups, HEAD_DIM)
    keys_all = key_cache.astype(jnp.float32).reshape(SEQS, CACHE_LEN, KV_HEADS, HEAD_DIM)
    values_all = value_cache.astype(jnp.float32).reshape(SEQS, CACHE_LEN, KV_HEADS, HEAD_DIM)
    inverse = 1.0 / math.sqrt(HEAD_DIM)
    scores = jnp.einsum('bkgd,bpkd->bkgp', grouped, keys_all) * inverse
    usable = (jnp.arange(CACHE_LEN, dtype=jnp.int32)[None, :] < lengths[:, None])[:, None, None, :]
    own_score = lax.optimization_barrier(jnp.sum(grouped * new_keys.astype(jnp.float32)[:, :, None, :], -1)) * inverse
    highest = jnp.maximum(lax.optimization_barrier(jnp.max(jnp.where(usable, scores, -1e+30), -1)), own_score)
    weights = jnp.exp(jnp.where(usable, scores - highest[..., None], -1e+30))
    own_weight = jnp.exp(own_score - highest)
    total = lax.optimization_barrier(jnp.sum(weights, -1)) + own_weight
    mixture = jnp.einsum('bkgp,bpkd->bkgd', weights, values_all) + own_weight[..., None] * new_values[:, :, None, :]
    attended = (mixture / total[..., None]).reshape(SEQS, q_width).astype(jnp.bfloat16)
    mixed_out = (widened + jnp.dot(attended, wo, preferred_element_type=jnp.float32)).astype(jnp.bfloat16)
    return (mixed_out, wqkv_new)
```

```python
import math

import jax
import jax.numpy as jnp
from jax import lax
from jax.experimental import pallas as pl
from jax.experimental.pallas import tpu as pltpu
from jax.sharding import PartitionSpec as P

HEADS = 64
KV_HEADS = 8
HEAD_DIM = 128
RANKS = 8
ROW_BLOCKS = 16
PER_SECTION_TP = 4
CHUNK_ROWS = 16
AHEAD = 4
MESH = pl.DeviceIdType.MESH
CONTRACT_LAST = (((1,), (1,)), ((), ()))


def layer_kernel(
    sections,
    hidden_in,
    gain_in,
    w_in,
    wo_in,
    key_in,
    value_in,
    lengths_in,
    order_in,
    mixed_out,
    new_out,
    hidden,
    gain,
    weight,
    held,
    wo,
    keys,
    values,
    lengths,
    order,
    places,
    normed,
    own_rows,
    x1,
    units,
    raw,
    turned,
    own_q,
    new_k,
    new_v,
    mask,
    mixes,
    parts,
    x2,
    merged,
    x3,
    attended,
    shares,
    x4,
    x5,
    x6,
    moved,
    load_sems,
    bulk_send,
    bulk_recv,
    cross_send,
    cross_recv,
    side_send,
    side_recv,
):
    members = RANKS
    replica = lax.axis_index("replica")
    tp = lax.axis_index("tp")
    sub = lax.axis_index("sub")
    section = tp // PER_SECTION_TP
    column = lax.rem(tp, PER_SECTION_TP)
    member = column * 2 + sub
    rank = section * members + member

    seqs, width = hidden.shape
    cols_dev = held.shape[1]
    rows_old = held.shape[2]
    per_section = ROW_BLOCKS // sections
    block_rows = rows_old // per_section
    unit_count = weight.shape[0]
    positions = keys.shape[1]
    own_heads = own_q.shape[1] // seqs
    head_rows = own_heads * seqs
    chunk_count = cols_dev // CHUNK_ROWS
    piece_count = chunk_count * (sections - 1)
    inverse = 1.0 / math.sqrt(HEAD_DIM)
    groups = HEADS // KV_HEADS
    share = width // members

    def cross_peer(off):
        other = lax.rem(section + off, sections)
        return other, (replica, other * PER_SECTION_TP + column, sub)

    def side_peer(off):
        other = lax.rem(member + off, members)
        return other, (replica, section * PER_SECTION_TP + other // 2, lax.rem(other, 2))

    barrier = pltpu.get_barrier_semaphore()
    for off in range(1, sections):
        pl.semaphore_signal(barrier, inc=1, device_id=cross_peer(off)[1], device_id_type=MESH)
    for off in range(1, members):
        pl.semaphore_signal(barrier, inc=1, device_id=side_peer(off)[1], device_id_type=MESH)

    own_start = pl.multiple_of(section * cols_dev, CHUNK_ROWS)
    loads = [
        pltpu.make_async_copy(source, target, load_sems.at[index])
        for index, (source, target) in enumerate(
            (
                (hidden_in, hidden),
                (gain_in, gain),
                (order_in, order),
                (lengths_in, lengths),
                (w_in.at[0, 0], weight),
                (key_in, keys),
                (value_in, values),
                (wo_in, wo),
                (w_in.at[0, 0, pl.ds(own_start, cols_dev)], held.at[section]),
            )
        )
    ]
    for load in loads:
        load.start()
    pl.semaphore_wait(barrier, sections - 1 + members - 1)

    def piece(index, arriving):
        chunk = index // (sections - 1)
        off = lax.rem(index, sections - 1) + 1
        other, peer = cross_peer(off)
        start = pl.multiple_of(chunk * CHUNK_ROWS, CHUNK_ROWS)
        slot = lax.rem(section + sections - off, sections) if arriving else section
        return pltpu.make_async_remote_copy(
            src_ref=w_in.at[
                0, 0, pl.ds(pl.multiple_of(other * cols_dev + start, CHUNK_ROWS), CHUNK_ROWS)
            ],
            dst_ref=held.at[slot, pl.ds(start, CHUNK_ROWS)],
            send_sem=bulk_send.at[index],
            recv_sem=bulk_recv.at[index],
            device_id=peer,
            device_id_type=MESH,
        )

    queued = [0]

    def queue(count):
        first = queued[0]
        last = min(first + count, piece_count)
        queued[0] = last
        if last > first:
            lax.fori_loop(first, last, lambda index, _: piece(index, False).start(), None)

    sent = []

    def cross_swap(step, source_of, target):
        def copy(off, arriving):
            other, peer = cross_peer(off)
            slot = lax.rem(section + sections - off, sections) if arriving else section
            return pltpu.make_async_remote_copy(
                src_ref=source_of(other),
                dst_ref=target.at[slot],
                send_sem=cross_send.at[step, off - 1],
                recv_sem=cross_recv.at[step, off - 1],
                device_id=peer,
                device_id_type=MESH,
            )

        for off in range(1, sections):
            outgoing = copy(off, False)
            outgoing.start()
            sent.append(outgoing)
        return lambda: [copy(off, True).wait_recv() for off in range(1, sections)]

    def side_swap(step, source_of, target):
        def copy(off, arriving):
            other, peer = side_peer(off)
            slot = lax.rem(member + members - off, members) if arriving else member
            return pltpu.make_async_remote_copy(
                src_ref=source_of(other),
                dst_ref=target.at[slot],
                send_sem=side_send.at[step, off - 1],
                recv_sem=side_recv.at[step, off - 1],
                device_id=peer,
                device_id_type=MESH,
            )

        for off in range(1, members):
            outgoing = copy(off, False)
            outgoing.start()
            sent.append(outgoing)
        return lambda: [copy(off, True).wait_recv() for off in range(1, members)]

    queue(AHEAD)

    for load in loads[:4]:
        load.wait()
    widened = hidden[...].astype(jnp.float32)
    factor = lax.rsqrt(jnp.mean(widened * widened, -1, keepdims=True) + 1e-05)
    rounded = (widened * factor * gain[...]).astype(jnp.bfloat16).astype(jnp.float32)
    for block in range(ROW_BLOCKS):
        normed[block] = rounded[:, block * block_rows : (block + 1) * block_rows]
    for slot in range(per_section):
        own_rows[:, slot * block_rows : (slot + 1) * block_rows] = normed[
            order[section * per_section + slot]
        ]
    loads[4].wait()
    rows = own_rows[...].astype(jnp.bfloat16)
    tile = 256

    def project(step, _):
        start = pl.multiple_of(step * tile, tile)
        x1[section, :, pl.ds(start, tile)] = lax.dot_general(
            rows, weight[pl.ds(start, tile), :], CONTRACT_LAST, preferred_element_type=jnp.float32
        )

    lax.fori_loop(0, unit_count // tile, project, None)
    arrive = cross_swap(0, lambda other: x1.at[section], x1)
    queue(AHEAD)

    row_index = lax.broadcasted_iota(jnp.int32, (8, HEAD_DIM), 0)
    lane_index = lax.broadcasted_iota(jnp.int32, (8, HEAD_DIM), 1)

    def by_seq(seq_of_row):
        picked = jnp.full(seq_of_row.shape, lengths[0], jnp.int32)
        for seq in range(1, seqs):
            picked = jnp.where(seq_of_row == seq, lengths[seq], picked)
        return picked

    half = HEAD_DIM // 2
    pair = jnp.where(lane_index < half, lane_index, lane_index - half).astype(jnp.float32)
    freqs = jnp.exp(pair * (-2.0 * math.log(500000.0) / HEAD_DIM))
    angles = by_seq(lax.rem(row_index, seqs)).astype(jnp.float32) * freqs
    cosine = jnp.cos(angles)
    sine = jnp.where(lane_index < half, -jnp.sin(angles), jnp.sin(angles))

    wide = (groups * seqs, seqs * positions)
    seq_of_row = lax.rem(lax.broadcasted_iota(jnp.int32, wide, 0), seqs)
    at = lax.broadcasted_iota(jnp.int32, wide, 1)
    usable = (at // positions == seq_of_row) & (
        rank * positions + lax.rem(at, positions) < by_seq(seq_of_row)
    )
    mask[...] = jnp.where(usable, 1.0, 0.0)

    def find(block, _):
        place = jnp.int32(0)
        for old in range(ROW_BLOCKS):
            place = jnp.where(order[old] == block, old, place)
        places[block] = place

    lax.fori_loop(0, ROW_BLOCKS, find, None)

    arrive()
    total = x1[0]
    for other in range(1, sections):
        total = total + x1[other]
    units[member] = total.astype(jnp.bfloat16).astype(jnp.float32)
    arrive = side_swap(0, lambda other: units.at[member], units)
    queue(AHEAD)
    for load in loads[5:]:
        load.wait()
    arrive()

    per_rank = unit_count // HEAD_DIM
    for head in range(HEADS + 2 * KV_HEADS):
        lane = (head % per_rank) * HEAD_DIM
        raw[head * seqs : (head + 1) * seqs, :] = units[
            head // per_rank, :, lane : lane + HEAD_DIM
        ]

    def turn(step, _):
        start = pl.multiple_of(step * 8, 8)
        vectors = raw[pl.ds(start, 8), :]
        out = vectors * cosine + pltpu.roll(vectors, half, 1) * sine
        turned[pl.ds(start, 8), :] = out.astype(jnp.bfloat16).astype(jnp.float32)

    lax.fori_loop(0, (HEADS + KV_HEADS) * seqs // 8, turn, None)
    for owner in range(sections * members):
        own_q[owner] = turned[owner * head_rows : (owner + 1) * head_rows, :]
    for head in range(KV_HEADS):
        key_row = (HEADS + head) * seqs
        value_row = (HEADS + KV_HEADS + head) * seqs
        for copy in range(own_heads):
            new_k[head, copy * seqs : (copy + 1) * seqs, :] = turned[key_row : key_row + seqs, :]
            new_v[head, copy * seqs : (copy + 1) * seqs, :] = raw[value_row : value_row + seqs, :]

    owners = groups // own_heads
    stat_lane = lax.broadcasted_iota(jnp.int32, (groups * seqs, HEAD_DIM), 1)

    def attend(head, _):
        lane = pl.ds(pl.multiple_of(head * HEAD_DIM, HEAD_DIM), HEAD_DIM)
        row = pl.multiple_of(head * groups * seqs, groups * seqs)
        query = turned[pl.ds(row, groups * seqs), :].astype(jnp.bfloat16)
        key = keys[:, :, lane].reshape(seqs * positions, HEAD_DIM)
        value = values[:, :, lane].reshape(seqs * positions, HEAD_DIM)
        open_ = mask[...] > 0.5
        scores = (
            lax.dot_general(query, key, CONTRACT_LAST, preferred_element_type=jnp.float32)
            * inverse
        )
        top = jnp.max(jnp.where(open_, scores, -1e30), -1, keepdims=True)
        weights = jnp.exp(jnp.where(open_, scores - top, -1e30))
        summed = jnp.sum(weights, -1, keepdims=True)
        high = weights.astype(jnp.bfloat16)
        low = (weights - high.astype(jnp.float32)).astype(jnp.bfloat16)
        mixes[:, :HEAD_DIM] = jnp.dot(
            high, value, preferred_element_type=jnp.float32
        ) + jnp.dot(low, value, preferred_element_type=jnp.float32)
        mixes[:, HEAD_DIM:] = jnp.where(stat_lane < half, top, summed)
        for index in range(owners):
            owner = head * owners + index
            parts[lax.rem(owner, members), owner // members] = mixes[
                index * head_rows : (index + 1) * head_rows, :
            ]

    lax.fori_loop(0, KV_HEADS, attend, None)
    arrive = side_swap(1, lambda other: parts.at[other], x2)
    x2[member] = parts[member]
    queue(AHEAD)
    arrive()

    def combined(refs):
        best = refs[0][:, HEAD_DIM : HEAD_DIM + 1]
        for ref in refs[1:]:
            best = jnp.maximum(best, ref[:, HEAD_DIM : HEAD_DIM + 1])
        mix = jnp.zeros((head_rows, HEAD_DIM), jnp.float32)
        summed = jnp.zeros((head_rows, 1), jnp.float32)
        for ref in refs:
            scale = jnp.exp(ref[:, HEAD_DIM : HEAD_DIM + 1] - best)
            mix = mix + ref[:, :HEAD_DIM] * scale
            summed = summed + ref[:, HEAD_DIM + half : HEAD_DIM + half + 1] * scale
        return best, summed, mix

    own_lane = lax.broadcasted_iota(jnp.int32, (head_rows, HEAD_DIM), 1)
    for other in range(sections):
        best, summed, mix = combined([x2[source, other] for source in range(members)])
        merged[other, :, :HEAD_DIM] = mix
        merged[other, :, HEAD_DIM:] = jnp.where(own_lane < half, best, summed)
    arrive = cross_swap(1, lambda other: merged.at[other], x3)
    x3[section] = merged[section]
    queue(AHEAD)
    arrive()

    best, summed, mix = combined([x3[source] for source in range(sections)])
    kv_head = rank * own_heads // groups
    own_score = jnp.sum(own_q[rank] * new_k[kv_head], -1, keepdims=True) * inverse
    highest = jnp.maximum(best, own_score)
    old_scale = jnp.exp(best - highest)
    own_weight = jnp.exp(own_score - highest)
    numerator = mix * old_scale + own_weight * new_v[kv_head]
    denominator = summed * old_scale + own_weight
    attended[...] = numerator / denominator
    flat = jnp.concatenate(
        [attended[head * seqs : (head + 1) * seqs, :] for head in range(own_heads)], -1
    ).astype(jnp.bfloat16)

    def give(other, _):
        lane = pl.ds(pl.multiple_of(other * share, share), share)
        shares[other] = jnp.dot(flat, wo[:, lane], preferred_element_type=jnp.float32)

    lax.fori_loop(0, members, give, None)
    arrive = side_swap(2, lambda other: shares.at[other], x4)
    x4[member] = shares[member]
    queue(AHEAD)
    arrive()

    total = x4[0]
    for other in range(1, members):
        total = total + x4[other]
    x5[section] = total
    arrive = cross_swap(2, lambda other: x5.at[section], x5)
    queue(AHEAD)
    arrive()

    total = hidden[:, pl.ds(pl.multiple_of(member * share, share), share)].astype(jnp.float32)
    product = x5[0]
    for other in range(1, sections):
        product = product + x5[other]
    x6[member] = (total + product).astype(jnp.bfloat16).astype(jnp.float32)
    arrive = side_swap(3, lambda other: x6.at[member], x6)
    queue(piece_count)
    arrive()
    for other in range(members):
        mixed_out[:, other * share : (other + 1) * share] = x6[other].astype(jnp.bfloat16)

    def place(chunk, _):
        for off in range(1, sections):
            piece(chunk * (sections - 1) + off - 1, True).wait_recv()
        start = pl.multiple_of(chunk * CHUNK_ROWS, CHUNK_ROWS)
        for old in range(ROW_BLOCKS):
            first = old % per_section * block_rows
            moved[old] = held[
                old // per_section, pl.ds(start, CHUNK_ROWS), first : first + block_rows
            ]
        for block in range(ROW_BLOCKS):
            new_out[0, 0, pl.ds(start, CHUNK_ROWS), block * block_rows : (block + 1) * block_rows] = (
                moved[places[block]]
            )

    lax.fori_loop(0, chunk_count, place, None)

    for outgoing in sent:
        outgoing.wait_send()
    lax.fori_loop(0, piece_count, lambda index, _: piece(index, False).wait_send(), None)


def shards(hidden_in, norm_gain, wqkv_old, wo, key_cache, value_cache, lengths, section_order):
    sections = lax.axis_size("tp") // PER_SECTION_TP
    members = PER_SECTION_TP * lax.axis_size("sub")
    seqs, width = hidden_in.shape
    unit_count, rows_old = wqkv_old.shape[2:]
    cols_dev = unit_count // sections
    block_rows = width // ROW_BLOCKS
    positions = key_cache.shape[1]
    own_heads = wo.shape[0] // HEAD_DIM
    head_rows = own_heads * seqs
    share = width // members
    pieces = cols_dev // CHUNK_ROWS * (sections - 1)
    f32, bf16 = jnp.float32, jnp.bfloat16
    heads = HEADS + 2 * KV_HEADS

    def kernel(*refs):
        layer_kernel(sections, *refs)

    scratch = [
        pltpu.VMEM(hidden_in.shape, bf16),
        pltpu.VMEM((1, width), f32),
        pltpu.VMEM((unit_count, rows_old), bf16),
        pltpu.VMEM((sections, cols_dev, rows_old), bf16),
        pltpu.VMEM(wo.shape, bf16),
        pltpu.VMEM(key_cache.shape, bf16),
        pltpu.VMEM(value_cache.shape, bf16),
        pltpu.SMEM(lengths.shape, jnp.int32),
        pltpu.SMEM(section_order.shape, jnp.int32),
        pltpu.SMEM(section_order.shape, jnp.int32),
        pltpu.VMEM((ROW_BLOCKS, seqs, block_rows), f32),
        pltpu.VMEM((seqs, rows_old), f32),
        pltpu.VMEM((sections, seqs, unit_count), f32),
        pltpu.VMEM((members, seqs, unit_count), f32),
        pltpu.VMEM((heads * seqs, HEAD_DIM), f32),
        pltpu.VMEM((heads * seqs, HEAD_DIM), f32),
        pltpu.VMEM((sections * members, head_rows, HEAD_DIM), f32),
        pltpu.VMEM((KV_HEADS, head_rows, HEAD_DIM), f32),
        pltpu.VMEM((KV_HEADS, head_rows, HEAD_DIM), f32),
        pltpu.VMEM((HEADS // KV_HEADS * seqs, seqs * positions), f32),
        pltpu.VMEM((HEADS // KV_HEADS * seqs, 2 * HEAD_DIM), f32),
        pltpu.VMEM((members, sections, head_rows, 2 * HEAD_DIM), f32),
        pltpu.VMEM((members, sections, head_rows, 2 * HEAD_DIM), f32),
        pltpu.VMEM((sections, head_rows, 2 * HEAD_DIM), f32),
        pltpu.VMEM((sections, head_rows, 2 * HEAD_DIM), f32),
        pltpu.VMEM((head_rows, HEAD_DIM), f32),
        pltpu.VMEM((members, seqs, share), f32),
        pltpu.VMEM((members, seqs, share), f32),
        pltpu.VMEM((sections, seqs, share), f32),
        pltpu.VMEM((members, seqs, share), f32),
        pltpu.VMEM((ROW_BLOCKS, CHUNK_ROWS, block_rows), bf16),
        pltpu.SemaphoreType.DMA((9,)),
        pltpu.SemaphoreType.DMA((pieces,)),
        pltpu.SemaphoreType.DMA((pieces,)),
        pltpu.SemaphoreType.DMA((3, sections - 1)),
        pltpu.SemaphoreType.DMA((3, sections - 1)),
        pltpu.SemaphoreType.DMA((4, members - 1)),
        pltpu.SemaphoreType.DMA((4, members - 1)),
    ]
    with jax.named_scope("layer"):
        return pl.pallas_call(
            kernel,
            out_shape=(
                pltpu.VMEM((seqs, width), bf16),
                pltpu.VMEM((1, 1, cols_dev, width), bf16),
            ),
            in_specs=[pl.BlockSpec(memory_space=pltpu.HBM)] * 8,
            out_specs=(pl.BlockSpec(memory_space=pltpu.VMEM), pl.BlockSpec(memory_space=pltpu.VMEM)),
            scratch_shapes=scratch,
            compiler_params=pltpu.CompilerParams(
                collective_id=0, has_side_effects=True, vmem_limit_bytes=45 * 2**20
            ),
        )(
            hidden_in,
            norm_gain.reshape(1, width),
            wqkv_old,
            wo,
            key_cache,
            value_cache,
            lengths,
            section_order,
        )


def solution(mesh):
    placed = (
        P("replica", None),
        P("replica"),
        P(("replica", "tp"), "sub", None, None),
        P(("replica", "tp", "sub"), None),
        P("replica", ("tp", "sub"), None),
        P("replica", ("tp", "sub"), None),
        P("replica"),
        P("replica"),
    )
    return jax.shard_map(
        shards,
        mesh=mesh,
        in_specs=placed,
        out_specs=(P("replica", None), P(("replica", "tp"), "sub", None, None)),
        check_vma=False,
    )
```

```python
import math

import jax
import jax.numpy as jnp
from jax import lax
from jax.experimental import pallas as pl
from jax.experimental.pallas import tpu as pltpu
from jax.sharding import PartitionSpec as P

HEADS = 64
KV_HEADS = 8
HEAD_DIM = 128
RANKS = 8
ROW_BLOCKS = 16
PER_SECTION_TP = 4
CHUNK_ROWS = 16
AHEAD = 6
MESH = pl.DeviceIdType.MESH
CONTRACT_LAST = (((1,), (1,)), ((), ()))


def layer_kernel(
    sections,
    hidden_in,
    gain_in,
    w_in,
    wo_in,
    key_in,
    value_in,
    lengths_in,
    order_in,
    mixed_out,
    new_out,
    hidden,
    gain,
    weight,
    held,
    wo,
    keys,
    values,
    lengths,
    order,
    places,
    normed,
    own_rows,
    x1,
    units,
    raw,
    turned,
    own_q,
    new_k,
    new_v,
    mask,
    mixes,
    parts,
    x2,
    merged,
    x3,
    attended,
    shares,
    x4,
    x5,
    x6,
    moved,
    load_sems,
    bulk_send,
    bulk_recv,
    cross_send,
    cross_recv,
    side_send,
    side_recv,
    section_in,
):
    members = RANKS
    replica = lax.axis_index("replica")
    tp = lax.axis_index("tp")
    sub = lax.axis_index("sub")
    section = tp // PER_SECTION_TP
    column = lax.rem(tp, PER_SECTION_TP)
    member = column * 2 + sub
    rank = section * members + member

    seqs, width = hidden.shape
    cols_dev = held.shape[1]
    rows_old = held.shape[2]
    per_section = ROW_BLOCKS // sections
    block_rows = rows_old // per_section
    unit_count = weight.shape[0]
    positions = keys.shape[1]
    own_heads = own_q.shape[1] // seqs
    head_rows = own_heads * seqs
    chunk_count = cols_dev // CHUNK_ROWS
    piece_count = chunk_count * (sections - 1)
    inverse = 1.0 / math.sqrt(HEAD_DIM)
    groups = HEADS // KV_HEADS
    share = width // members

    def cross_peer(off):
        other = lax.rem(section + off, sections)
        return other, (replica, other * PER_SECTION_TP + column, sub)

    def side_peer(off):
        other = lax.rem(member + off, members)
        return other, (replica, section * PER_SECTION_TP + other // 2, lax.rem(other, 2))

    barrier = pltpu.get_barrier_semaphore()
    lower = members // 2
    in_lower = member < lower
    for off in range(1, sections):
        pl.semaphore_signal(barrier, inc=1, device_id=cross_peer(off)[1], device_id_type=MESH)
    for off in range(1, members):
        other, peer = side_peer(off)

        @pl.when(other < lower)
        def _():
            pl.semaphore_signal(barrier, inc=1, device_id=peer, device_id_type=MESH)

    own_start = pl.multiple_of(section * cols_dev, CHUNK_ROWS)
    loads = [
        pltpu.make_async_copy(source, target, load_sems.at[index])
        for index, (source, target) in enumerate(
            (
                (hidden_in, hidden),
                (gain_in, gain),
                (order_in, order),
                (lengths_in, lengths),
                (w_in.at[0, 0], weight),
                (key_in, keys),
                (value_in, values),
                (wo_in, wo),
                (w_in.at[0, 0, pl.ds(own_start, cols_dev)], held.at[section]),
            )
        )
    ]
    for load in loads:
        load.start()
    pl.semaphore_wait(barrier, sections - 1 + jnp.where(in_lower, members - 1, 0))

    @pl.when(in_lower)
    def _():
        pl.semaphore_signal(
            section_in, inc=1, device_id=side_peer(lower)[1], device_id_type=MESH
        )

    def piece(index, arriving):
        chunk = index // (sections - 1)
        off = lax.rem(index, sections - 1) + 1
        other, peer = cross_peer(off)
        start = pl.multiple_of(chunk * CHUNK_ROWS, CHUNK_ROWS)
        slot = lax.rem(section + sections - off, sections) if arriving else section
        return pltpu.make_async_remote_copy(
            src_ref=w_in.at[
                0, 0, pl.ds(pl.multiple_of(other * cols_dev + start, CHUNK_ROWS), CHUNK_ROWS)
            ],
            dst_ref=held.at[slot, pl.ds(start, CHUNK_ROWS)],
            send_sem=bulk_send.at[index],
            recv_sem=bulk_recv.at[index],
            device_id=peer,
            device_id_type=MESH,
        )

    queued = [0]

    def queue(count):
        first = queued[0]
        last = min(first + count, piece_count)
        queued[0] = last
        if last > first:
            lax.fori_loop(first, last, lambda index, _: piece(index, False).start(), None)

    sent = []

    def cross_swap(step, source_of, target):
        def copy(off, arriving):
            other, peer = cross_peer(off)
            slot = lax.rem(section + sections - off, sections) if arriving else section
            return pltpu.make_async_remote_copy(
                src_ref=source_of(other),
                dst_ref=target.at[slot],
                send_sem=cross_send.at[step, off - 1],
                recv_sem=cross_recv.at[step, off - 1],
                device_id=peer,
                device_id_type=MESH,
            )

        for off in range(1, sections):
            outgoing = copy(off, False)
            outgoing.start()
            sent.append(outgoing)
        return lambda: [copy(off, True).wait_recv() for off in range(1, sections)]

    def side_swap(step, source_of, target):
        def copy(off, arriving):
            other, peer = side_peer(off)
            slot = lax.rem(member + members - off, members) if arriving else member
            return pltpu.make_async_remote_copy(
                src_ref=source_of(other),
                dst_ref=target.at[slot],
                send_sem=side_send.at[step, off - 1],
                recv_sem=side_recv.at[step, off - 1],
                device_id=peer,
                device_id_type=MESH,
            )

        for off in range(1, members):
            outgoing = copy(off, False)
            outgoing.start()
            sent.append(outgoing)
        return lambda: [copy(off, True).wait_recv() for off in range(1, members)]

    queue(AHEAD)

    for load in loads[:4]:
        load.wait()
    widened = hidden[...].astype(jnp.float32)
    factor = lax.rsqrt(jnp.mean(widened * widened, -1, keepdims=True) + 1e-05)
    rounded = (widened * factor * gain[...]).astype(jnp.bfloat16).astype(jnp.float32)
    for block in range(ROW_BLOCKS):
        normed[block] = rounded[:, block * block_rows : (block + 1) * block_rows]
    for slot in range(per_section):
        own_rows[:, slot * block_rows : (slot + 1) * block_rows] = normed[
            order[section * per_section + slot]
        ]
    loads[4].wait()
    rows = own_rows[...].astype(jnp.bfloat16)
    tile = 256

    def project(step, _):
        start = pl.multiple_of(step * tile, tile)
        x1[section, :, pl.ds(start, tile)] = lax.dot_general(
            rows, weight[pl.ds(start, tile), :], CONTRACT_LAST, preferred_element_type=jnp.float32
        )

    lax.fori_loop(0, unit_count // tile, project, None)
    arrive = cross_swap(0, lambda other: x1.at[section], x1)
    queue(AHEAD)

    row_index = lax.broadcasted_iota(jnp.int32, (8, HEAD_DIM), 0)
    lane_index = lax.broadcasted_iota(jnp.int32, (8, HEAD_DIM), 1)

    def by_seq(seq_of_row):
        picked = jnp.full(seq_of_row.shape, lengths[0], jnp.int32)
        for seq in range(1, seqs):
            picked = jnp.where(seq_of_row == seq, lengths[seq], picked)
        return picked

    half = HEAD_DIM // 2
    pair = jnp.where(lane_index < half, lane_index, lane_index - half).astype(jnp.float32)
    freqs = jnp.exp(pair * (-2.0 * math.log(500000.0) / HEAD_DIM))
    angles = by_seq(lax.rem(row_index, seqs)).astype(jnp.float32) * freqs
    cosine = jnp.cos(angles)
    sine = jnp.where(lane_index < half, -jnp.sin(angles), jnp.sin(angles))

    wide = (groups * seqs, seqs * positions)
    seq_of_row = lax.rem(lax.broadcasted_iota(jnp.int32, wide, 0), seqs)
    at = lax.broadcasted_iota(jnp.int32, wide, 1)
    usable = (at // positions == seq_of_row) & (
        rank * positions + lax.rem(at, positions) < by_seq(seq_of_row)
    )
    mask[...] = jnp.where(usable, 1.0, 0.0)

    def find(block, _):
        place = jnp.int32(0)
        for old in range(ROW_BLOCKS):
            place = jnp.where(order[old] == block, old, place)
        places[block] = place

    lax.fori_loop(0, ROW_BLOCKS, find, None)

    arrive()
    total = x1[0]
    for other in range(1, sections):
        total = total + x1[other]
    units[member] = total.astype(jnp.bfloat16).astype(jnp.float32)

    @pl.when(jnp.logical_not(in_lower))
    def _():
        pl.semaphore_wait(section_in, 1)

    arrive = side_swap(0, lambda other: units.at[member], units)
    queue(AHEAD)
    for load in loads[5:]:
        load.wait()
    arrive()

    per_rank = unit_count // HEAD_DIM
    for head in range(HEADS + 2 * KV_HEADS):
        lane = (head % per_rank) * HEAD_DIM
        raw[head * seqs : (head + 1) * seqs, :] = units[
            head // per_rank, :, lane : lane + HEAD_DIM
        ]

    def turn(step, _):
        start = pl.multiple_of(step * 8, 8)
        vectors = raw[pl.ds(start, 8), :]
        out = vectors * cosine + pltpu.roll(vectors, half, 1) * sine
        turned[pl.ds(start, 8), :] = out.astype(jnp.bfloat16).astype(jnp.float32)

    lax.fori_loop(0, (HEADS + KV_HEADS) * seqs // 8, turn, None)
    for owner in range(sections * members):
        own_q[owner] = turned[owner * head_rows : (owner + 1) * head_rows, :]
    for head in range(KV_HEADS):
        key_row = (HEADS + head) * seqs
        value_row = (HEADS + KV_HEADS + head) * seqs
        for copy in range(own_heads):
            new_k[head, copy * seqs : (copy + 1) * seqs, :] = turned[key_row : key_row + seqs, :]
            new_v[head, copy * seqs : (copy + 1) * seqs, :] = raw[value_row : value_row + seqs, :]

    owners = groups // own_heads
    stat_lane = lax.broadcasted_iota(jnp.int32, (groups * seqs, HEAD_DIM), 1)

    def attend(head, _):
        lane = pl.ds(pl.multiple_of(head * HEAD_DIM, HEAD_DIM), HEAD_DIM)
        row = pl.multiple_of(head * groups * seqs, groups * seqs)
        query = turned[pl.ds(row, groups * seqs), :].astype(jnp.bfloat16)
        key = keys[:, :, lane].reshape(seqs * positions, HEAD_DIM)
        value = values[:, :, lane].reshape(seqs * positions, HEAD_DIM)
        open_ = mask[...] > 0.5
        scores = (
            lax.dot_general(query, key, CONTRACT_LAST, preferred_element_type=jnp.float32)
            * inverse
        )
        top = jnp.max(jnp.where(open_, scores, -1e30), -1, keepdims=True)
        weights = jnp.exp(jnp.where(open_, scores - top, -1e30))
        summed = jnp.sum(weights, -1, keepdims=True)
        high = weights.astype(jnp.bfloat16)
        low = (weights - high.astype(jnp.float32)).astype(jnp.bfloat16)
        mixes[:, :HEAD_DIM] = jnp.dot(
            high, value, preferred_element_type=jnp.float32
        ) + jnp.dot(low, value, preferred_element_type=jnp.float32)
        mixes[:, HEAD_DIM:] = jnp.where(stat_lane < half, top, summed)
        for index in range(owners):
            owner = head * owners + index
            parts[lax.rem(owner, members), owner // members] = mixes[
                index * head_rows : (index + 1) * head_rows, :
            ]

    lax.fori_loop(0, KV_HEADS, attend, None)
    arrive = side_swap(1, lambda other: parts.at[other], x2)
    x2[member] = parts[member]
    queue(AHEAD)
    arrive()

    def combined(refs):
        best = refs[0][:, HEAD_DIM : HEAD_DIM + 1]
        for ref in refs[1:]:
            best = jnp.maximum(best, ref[:, HEAD_DIM : HEAD_DIM + 1])
        mix = jnp.zeros((head_rows, HEAD_DIM), jnp.float32)
        summed = jnp.zeros((head_rows, 1), jnp.float32)
        for ref in refs:
            scale = jnp.exp(ref[:, HEAD_DIM : HEAD_DIM + 1] - best)
            mix = mix + ref[:, :HEAD_DIM] * scale
            summed = summed + ref[:, HEAD_DIM + half : HEAD_DIM + half + 1] * scale
        return best, summed, mix

    own_lane = lax.broadcasted_iota(jnp.int32, (head_rows, HEAD_DIM), 1)
    for other in range(sections):
        best, summed, mix = combined([x2[source, other] for source in range(members)])
        merged[other, :, :HEAD_DIM] = mix
        merged[other, :, HEAD_DIM:] = jnp.where(own_lane < half, best, summed)
    arrive = cross_swap(1, lambda other: merged.at[other], x3)
    x3[section] = merged[section]
    queue(AHEAD)
    arrive()

    best, summed, mix = combined([x3[source] for source in range(sections)])
    kv_head = rank * own_heads // groups
    own_score = jnp.sum(own_q[rank] * new_k[kv_head], -1, keepdims=True) * inverse
    highest = jnp.maximum(best, own_score)
    old_scale = jnp.exp(best - highest)
    own_weight = jnp.exp(own_score - highest)
    numerator = mix * old_scale + own_weight * new_v[kv_head]
    denominator = summed * old_scale + own_weight
    attended[...] = numerator / denominator
    flat = jnp.concatenate(
        [attended[head * seqs : (head + 1) * seqs, :] for head in range(own_heads)], -1
    ).astype(jnp.bfloat16)

    def give(other, _):
        lane = pl.ds(pl.multiple_of(other * share, share), share)
        shares[other] = jnp.dot(flat, wo[:, lane], preferred_element_type=jnp.float32)

    lax.fori_loop(0, members, give, None)
    arrive = side_swap(2, lambda other: shares.at[other], x4)
    x4[member] = shares[member]
    queue(AHEAD)
    arrive()

    total = x4[0]
    for other in range(1, members):
        total = total + x4[other]
    x5[section] = total
    arrive = cross_swap(2, lambda other: x5.at[section], x5)
    queue(AHEAD)
    arrive()

    total = hidden[:, pl.ds(pl.multiple_of(member * share, share), share)].astype(jnp.float32)
    product = x5[0]
    for other in range(1, sections):
        product = product + x5[other]
    x6[member] = (total + product).astype(jnp.bfloat16).astype(jnp.float32)
    arrive = side_swap(3, lambda other: x6.at[member], x6)
    queue(piece_count)
    arrive()
    for other in range(members):
        mixed_out[:, other * share : (other + 1) * share] = x6[other].astype(jnp.bfloat16)

    def place(chunk, _):
        for off in range(1, sections):
            piece(chunk * (sections - 1) + off - 1, True).wait_recv()
        start = pl.multiple_of(chunk * CHUNK_ROWS, CHUNK_ROWS)
        for old in range(ROW_BLOCKS):
            first = old % per_section * block_rows
            moved[old] = held[
                old // per_section, pl.ds(start, CHUNK_ROWS), first : first + block_rows
            ]
        for block in range(ROW_BLOCKS):
            new_out[0, 0, pl.ds(start, CHUNK_ROWS), block * block_rows : (block + 1) * block_rows] = (
                moved[places[block]]
            )

    lax.fori_loop(0, chunk_count, place, None)

    for outgoing in sent:
        outgoing.wait_send()
    lax.fori_loop(0, piece_count, lambda index, _: piece(index, False).wait_send(), None)


def shards(hidden_in, norm_gain, wqkv_old, wo, key_cache, value_cache, lengths, section_order):
    sections = lax.axis_size("tp") // PER_SECTION_TP
    members = PER_SECTION_TP * lax.axis_size("sub")
    seqs, width = hidden_in.shape
    unit_count, rows_old = wqkv_old.shape[2:]
    cols_dev = unit_count // sections
    block_rows = width // ROW_BLOCKS
    positions = key_cache.shape[1]
    own_heads = wo.shape[0] // HEAD_DIM
    head_rows = own_heads * seqs
    share = width // members
    pieces = cols_dev // CHUNK_ROWS * (sections - 1)
    f32, bf16 = jnp.float32, jnp.bfloat16
    heads = HEADS + 2 * KV_HEADS

    def kernel(*refs):
        layer_kernel(sections, *refs)

    scratch = [
        pltpu.VMEM(hidden_in.shape, bf16),
        pltpu.VMEM((1, width), f32),
        pltpu.VMEM((unit_count, rows_old), bf16),
        pltpu.VMEM((sections, cols_dev, rows_old), bf16),
        pltpu.VMEM(wo.shape, bf16),
        pltpu.VMEM(key_cache.shape, bf16),
        pltpu.VMEM(value_cache.shape, bf16),
        pltpu.SMEM(lengths.shape, jnp.int32),
        pltpu.SMEM(section_order.shape, jnp.int32),
        pltpu.SMEM(section_order.shape, jnp.int32),
        pltpu.VMEM((ROW_BLOCKS, seqs, block_rows), f32),
        pltpu.VMEM((seqs, rows_old), f32),
        pltpu.VMEM((sections, seqs, unit_count), f32),
        pltpu.VMEM((members, seqs, unit_count), f32),
        pltpu.VMEM((heads * seqs, HEAD_DIM), f32),
        pltpu.VMEM((heads * seqs, HEAD_DIM), f32),
        pltpu.VMEM((sections * members, head_rows, HEAD_DIM), f32),
        pltpu.VMEM((KV_HEADS, head_rows, HEAD_DIM), f32),
        pltpu.VMEM((KV_HEADS, head_rows, HEAD_DIM), f32),
        pltpu.VMEM((HEADS // KV_HEADS * seqs, seqs * positions), f32),
        pltpu.VMEM((HEADS // KV_HEADS * seqs, 2 * HEAD_DIM), f32),
        pltpu.VMEM((members, sections, head_rows, 2 * HEAD_DIM), f32),
        pltpu.VMEM((members, sections, head_rows, 2 * HEAD_DIM), f32),
        pltpu.VMEM((sections, head_rows, 2 * HEAD_DIM), f32),
        pltpu.VMEM((sections, head_rows, 2 * HEAD_DIM), f32),
        pltpu.VMEM((head_rows, HEAD_DIM), f32),
        pltpu.VMEM((members, seqs, share), f32),
        pltpu.VMEM((members, seqs, share), f32),
        pltpu.VMEM((sections, seqs, share), f32),
        pltpu.VMEM((members, seqs, share), f32),
        pltpu.VMEM((ROW_BLOCKS, CHUNK_ROWS, block_rows), bf16),
        pltpu.SemaphoreType.DMA((9,)),
        pltpu.SemaphoreType.DMA((pieces,)),
        pltpu.SemaphoreType.DMA((pieces,)),
        pltpu.SemaphoreType.DMA((3, sections - 1)),
        pltpu.SemaphoreType.DMA((3, sections - 1)),
        pltpu.SemaphoreType.DMA((4, members - 1)),
        pltpu.SemaphoreType.DMA((4, members - 1)),
        pltpu.SemaphoreType.REGULAR,
    ]
    with jax.named_scope("layer"):
        return pl.pallas_call(
            kernel,
            out_shape=(
                pltpu.VMEM((seqs, width), bf16),
                pltpu.VMEM((1, 1, cols_dev, width), bf16),
            ),
            in_specs=[pl.BlockSpec(memory_space=pltpu.HBM)] * 8,
            out_specs=(pl.BlockSpec(memory_space=pltpu.VMEM), pl.BlockSpec(memory_space=pltpu.VMEM)),
            scratch_shapes=scratch,
            compiler_params=pltpu.CompilerParams(
                collective_id=0, has_side_effects=True, vmem_limit_bytes=45 * 2**20
            ),
        )(
            hidden_in,
            norm_gain.reshape(1, width),
            wqkv_old,
            wo,
            key_cache,
            value_cache,
            lengths,
            section_order,
        )


def solution(mesh):
    placed = (
        P("replica", None),
        P("replica"),
        P(("replica", "tp"), "sub", None, None),
        P(("replica", "tp", "sub"), None),
        P("replica", ("tp", "sub"), None),
        P("replica", ("tp", "sub"), None),
        P("replica"),
        P("replica"),
    )
    return jax.shard_map(
        shards,
        mesh=mesh,
        in_specs=placed,
        out_specs=(P("replica", None), P(("replica", "tp"), "sub", None, None)),
        check_vma=False,
    )
```

```python
import math

import jax
import jax.numpy as jnp
from jax import lax
from jax.experimental import pallas as pl
from jax.experimental.pallas import tpu as pltpu
from jax.sharding import PartitionSpec as P

HEADS = 64
KV_HEADS = 8
HEAD_DIM = 128
RANKS = 8
ROW_BLOCKS = 16
PER_SECTION_TP = 4
CHUNK_ROWS = 16
AHEAD = 4
WRITES = 4
MESH = pl.DeviceIdType.MESH
CONTRACT_LAST = (((1,), (1,)), ((), ()))


def layer_kernel(
    sections,
    hidden_in,
    gain_in,
    w_in,
    wo_in,
    key_in,
    value_in,
    lengths_in,
    order_in,
    mixed_out,
    new_out,
    hidden,
    gain,
    weight,
    held,
    wo,
    keys,
    values,
    lengths,
    order,
    places,
    normed,
    own_rows,
    x1,
    units,
    raw,
    turned,
    own_q,
    new_k,
    new_v,
    mask,
    mixes,
    parts,
    x2,
    merged,
    x3,
    attended,
    shares,
    x4,
    x5,
    x6,
    moved,
    load_sems,
    bulk_send,
    bulk_recv,
    cross_send,
    cross_recv,
    side_send,
    side_recv,
    section_in,
):
    members = RANKS
    replica = lax.axis_index("replica")
    tp = lax.axis_index("tp")
    sub = lax.axis_index("sub")
    section = tp // PER_SECTION_TP
    column = lax.rem(tp, PER_SECTION_TP)
    member = column * 2 + sub
    rank = section * members + member

    seqs, width = hidden.shape
    cols_dev = held.shape[1]
    rows_old = held.shape[2]
    per_section = ROW_BLOCKS // sections
    block_rows = rows_old // per_section
    unit_count = weight.shape[0]
    positions = keys.shape[1]
    own_heads = own_q.shape[1] // seqs
    head_rows = own_heads * seqs
    chunk_count = cols_dev // CHUNK_ROWS
    piece_count = chunk_count * (sections - 1)
    inverse = 1.0 / math.sqrt(HEAD_DIM)
    groups = HEADS // KV_HEADS
    share = width // members

    def cross_peer(off):
        other = lax.rem(section + off, sections)
        return other, (replica, other * PER_SECTION_TP + column, sub)

    def side_peer(off):
        other = lax.rem(member + off, members)
        return other, (replica, section * PER_SECTION_TP + other // 2, lax.rem(other, 2))

    barrier = pltpu.get_barrier_semaphore()
    is_first = member == 0
    for off in range(1, sections):
        pl.semaphore_signal(barrier, inc=1, device_id=cross_peer(off)[1], device_id_type=MESH)

    @pl.when(jnp.logical_not(is_first))
    def _():
        pl.semaphore_signal(
            barrier,
            inc=1,
            device_id=(replica, section * PER_SECTION_TP, 0),
            device_id_type=MESH,
        )

    own_start = pl.multiple_of(section * cols_dev, CHUNK_ROWS)
    loads = [
        pltpu.make_async_copy(source, target, load_sems.at[index])
        for index, (source, target) in enumerate(
            (
                (hidden_in, hidden),
                (gain_in, gain),
                (order_in, order),
                (lengths_in, lengths),
                (w_in.at[0, 0], weight),
                (key_in, keys),
                (value_in, values),
                (wo_in, wo),
                (w_in.at[0, 0, pl.ds(own_start, cols_dev)], held.at[section]),
            )
        )
    ]
    for load in loads:
        load.start()
    pl.semaphore_wait(barrier, sections - 1 + jnp.where(is_first, members - 1, 0))

    @pl.when(is_first)
    def _():
        for off in range(1, members):
            pl.semaphore_signal(
                section_in, inc=1, device_id=side_peer(off)[1], device_id_type=MESH
            )

    def piece(index, arriving):
        chunk = index // (sections - 1)
        off = lax.rem(index, sections - 1) + 1
        other, peer = cross_peer(off)
        start = pl.multiple_of(chunk * CHUNK_ROWS, CHUNK_ROWS)
        slot = lax.rem(section + sections - off, sections) if arriving else section
        return pltpu.make_async_remote_copy(
            src_ref=w_in.at[
                0, 0, pl.ds(pl.multiple_of(other * cols_dev + start, CHUNK_ROWS), CHUNK_ROWS)
            ],
            dst_ref=held.at[slot, pl.ds(start, CHUNK_ROWS)],
            send_sem=bulk_send.at[index],
            recv_sem=bulk_recv.at[index],
            device_id=peer,
            device_id_type=MESH,
        )

    queued = [0]

    def queue(count):
        first = queued[0]
        last = min(first + count, piece_count)
        queued[0] = last
        if last > first:
            lax.fori_loop(first, last, lambda index, _: piece(index, False).start(), None)

    sent = []

    def cross_swap(step, source_of, target):
        def copy(off, arriving):
            other, peer = cross_peer(off)
            slot = lax.rem(section + sections - off, sections) if arriving else section
            return pltpu.make_async_remote_copy(
                src_ref=source_of(other),
                dst_ref=target.at[slot],
                send_sem=cross_send.at[step, off - 1],
                recv_sem=cross_recv.at[step, off - 1],
                device_id=peer,
                device_id_type=MESH,
            )

        for off in range(1, sections):
            outgoing = copy(off, False)
            outgoing.start()
            sent.append(outgoing)
        return lambda: [copy(off, True).wait_recv() for off in range(1, sections)]

    def side_swap(step, source_of, target):
        def copy(off, arriving):
            other, peer = side_peer(off)
            slot = lax.rem(member + members - off, members) if arriving else member
            return pltpu.make_async_remote_copy(
                src_ref=source_of(other),
                dst_ref=target.at[slot],
                send_sem=side_send.at[step, off - 1],
                recv_sem=side_recv.at[step, off - 1],
                device_id=peer,
                device_id_type=MESH,
            )

        for off in range(1, members):
            outgoing = copy(off, False)
            outgoing.start()
            sent.append(outgoing)
        return lambda: [copy(off, True).wait_recv() for off in range(1, members)]

    queue(AHEAD)

    for load in loads[:4]:
        load.wait()
    widened = hidden[...].astype(jnp.float32)
    factor = lax.rsqrt(jnp.mean(widened * widened, -1, keepdims=True) + 1e-05)
    rounded = (widened * factor * gain[...]).astype(jnp.bfloat16).astype(jnp.float32)
    for block in range(ROW_BLOCKS):
        normed[block] = rounded[:, block * block_rows : (block + 1) * block_rows]
    for slot in range(per_section):
        own_rows[:, slot * block_rows : (slot + 1) * block_rows] = normed[
            order[section * per_section + slot]
        ]
    loads[4].wait()
    rows = own_rows[...].astype(jnp.bfloat16)
    tile = 256

    def project(step, _):
        start = pl.multiple_of(step * tile, tile)
        x1[section, :, pl.ds(start, tile)] = lax.dot_general(
            rows, weight[pl.ds(start, tile), :], CONTRACT_LAST, preferred_element_type=jnp.float32
        )

    lax.fori_loop(0, unit_count // tile, project, None)
    arrive = cross_swap(0, lambda other: x1.at[section], x1)
    queue(AHEAD)

    row_index = lax.broadcasted_iota(jnp.int32, (8, HEAD_DIM), 0)
    lane_index = lax.broadcasted_iota(jnp.int32, (8, HEAD_DIM), 1)

    def by_seq(seq_of_row):
        picked = jnp.full(seq_of_row.shape, lengths[0], jnp.int32)
        for seq in range(1, seqs):
            picked = jnp.where(seq_of_row == seq, lengths[seq], picked)
        return picked

    half = HEAD_DIM // 2
    pair = jnp.where(lane_index < half, lane_index, lane_index - half).astype(jnp.float32)
    freqs = jnp.exp(pair * (-2.0 * math.log(500000.0) / HEAD_DIM))
    angles = by_seq(lax.rem(row_index, seqs)).astype(jnp.float32) * freqs
    cosine = jnp.cos(angles)
    sine = jnp.where(lane_index < half, -jnp.sin(angles), jnp.sin(angles))

    wide = (groups * seqs, seqs * positions)
    seq_of_row = lax.rem(lax.broadcasted_iota(jnp.int32, wide, 0), seqs)
    at = lax.broadcasted_iota(jnp.int32, wide, 1)
    usable = (at // positions == seq_of_row) & (
        rank * positions + lax.rem(at, positions) < by_seq(seq_of_row)
    )
    mask[...] = jnp.where(usable, 1.0, 0.0)

    def find(block, _):
        place = jnp.int32(0)
        for old in range(ROW_BLOCKS):
            place = jnp.where(order[old] == block, old, place)
        places[block] = place

    lax.fori_loop(0, ROW_BLOCKS, find, None)

    arrive()
    total = x1[0]
    for other in range(1, sections):
        total = total + x1[other]
    units[member] = total.astype(jnp.bfloat16).astype(jnp.float32)

    @pl.when(jnp.logical_not(is_first))
    def _():
        pl.semaphore_wait(section_in, 1)

    arrive = side_swap(0, lambda other: units.at[member], units)
    queue(AHEAD)
    for load in loads[5:]:
        load.wait()
    arrive()

    per_rank = unit_count // HEAD_DIM
    for head in range(HEADS + 2 * KV_HEADS):
        lane = (head % per_rank) * HEAD_DIM
        raw[head * seqs : (head + 1) * seqs, :] = units[
            head // per_rank, :, lane : lane + HEAD_DIM
        ]

    def turn(step, _):
        start = pl.multiple_of(step * 8, 8)
        vectors = raw[pl.ds(start, 8), :]
        out = vectors * cosine + pltpu.roll(vectors, half, 1) * sine
        turned[pl.ds(start, 8), :] = out.astype(jnp.bfloat16).astype(jnp.float32)

    lax.fori_loop(0, (HEADS + KV_HEADS) * seqs // 8, turn, None)
    for owner in range(sections * members):
        own_q[owner] = turned[owner * head_rows : (owner + 1) * head_rows, :]
    for head in range(KV_HEADS):
        key_row = (HEADS + head) * seqs
        value_row = (HEADS + KV_HEADS + head) * seqs
        for copy in range(own_heads):
            new_k[head, copy * seqs : (copy + 1) * seqs, :] = turned[key_row : key_row + seqs, :]
            new_v[head, copy * seqs : (copy + 1) * seqs, :] = raw[value_row : value_row + seqs, :]

    owners = groups // own_heads
    stat_lane = lax.broadcasted_iota(jnp.int32, (groups * seqs, HEAD_DIM), 1)

    def attend(head, _):
        lane = pl.ds(pl.multiple_of(head * HEAD_DIM, HEAD_DIM), HEAD_DIM)
        row = pl.multiple_of(head * groups * seqs, groups * seqs)
        query = turned[pl.ds(row, groups * seqs), :].astype(jnp.bfloat16)
        key = keys[:, :, lane].reshape(seqs * positions, HEAD_DIM)
        value = values[:, :, lane].reshape(seqs * positions, HEAD_DIM)
        open_ = mask[...] > 0.5
        scores = (
            lax.dot_general(query, key, CONTRACT_LAST, preferred_element_type=jnp.float32)
            * inverse
        )
        top = jnp.max(jnp.where(open_, scores, -1e30), -1, keepdims=True)
        weights = jnp.exp(jnp.where(open_, scores - top, -1e30))
        summed = jnp.sum(weights, -1, keepdims=True)
        high = weights.astype(jnp.bfloat16)
        low = (weights - high.astype(jnp.float32)).astype(jnp.bfloat16)
        mixes[:, :HEAD_DIM] = jnp.dot(
            high, value, preferred_element_type=jnp.float32
        ) + jnp.dot(low, value, preferred_element_type=jnp.float32)
        mixes[:, HEAD_DIM:] = jnp.where(stat_lane < half, top, summed)
        for index in range(owners):
            owner = head * owners + index
            parts[lax.rem(owner, members), owner // members] = mixes[
                index * head_rows : (index + 1) * head_rows, :
            ]

    lax.fori_loop(0, KV_HEADS, attend, None)
    arrive = side_swap(1, lambda other: parts.at[other], x2)
    x2[member] = parts[member]
    queue(AHEAD)
    arrive()

    def combined(refs):
        best = refs[0][:, HEAD_DIM : HEAD_DIM + 1]
        for ref in refs[1:]:
            best = jnp.maximum(best, ref[:, HEAD_DIM : HEAD_DIM + 1])
        mix = jnp.zeros((head_rows, HEAD_DIM), jnp.float32)
        summed = jnp.zeros((head_rows, 1), jnp.float32)
        for ref in refs:
            scale = jnp.exp(ref[:, HEAD_DIM : HEAD_DIM + 1] - best)
            mix = mix + ref[:, :HEAD_DIM] * scale
            summed = summed + ref[:, HEAD_DIM + half : HEAD_DIM + half + 1] * scale
        return best, summed, mix

    own_lane = lax.broadcasted_iota(jnp.int32, (head_rows, HEAD_DIM), 1)
    for other in range(sections):
        best, summed, mix = combined([x2[source, other] for source in range(members)])
        merged[other, :, :HEAD_DIM] = mix
        merged[other, :, HEAD_DIM:] = jnp.where(own_lane < half, best, summed)
    arrive = cross_swap(1, lambda other: merged.at[other], x3)
    x3[section] = merged[section]
    queue(AHEAD)
    arrive()

    best, summed, mix = combined([x3[source] for source in range(sections)])
    kv_head = rank * own_heads // groups
    own_score = jnp.sum(own_q[rank] * new_k[kv_head], -1, keepdims=True) * inverse
    highest = jnp.maximum(best, own_score)
    old_scale = jnp.exp(best - highest)
    own_weight = jnp.exp(own_score - highest)
    numerator = mix * old_scale + own_weight * new_v[kv_head]
    denominator = summed * old_scale + own_weight
    attended[...] = numerator / denominator
    flat = jnp.concatenate(
        [attended[head * seqs : (head + 1) * seqs, :] for head in range(own_heads)], -1
    ).astype(jnp.bfloat16)

    def give(other, _):
        lane = pl.ds(pl.multiple_of(other * share, share), share)
        shares[other] = jnp.dot(flat, wo[:, lane], preferred_element_type=jnp.float32)

    lax.fori_loop(0, members, give, None)
    arrive = side_swap(2, lambda other: shares.at[other], x4)
    x4[member] = shares[member]
    queue(AHEAD)
    arrive()

    total = x4[0]
    for other in range(1, members):
        total = total + x4[other]
    x5[section] = total
    arrive = cross_swap(2, lambda other: x5.at[section], x5)
    queue(AHEAD)
    arrive()

    total = hidden[:, pl.ds(pl.multiple_of(member * share, share), share)].astype(jnp.float32)
    product = x5[0]
    for other in range(1, sections):
        product = product + x5[other]
    x6[member] = (total + product).astype(jnp.bfloat16).astype(jnp.float32)
    arrive = side_swap(3, lambda other: x6.at[member], x6)
    queue(piece_count)
    arrive()
    for other in range(members):
        mixed_out[:, other * share : (other + 1) * share] = x6[other].astype(jnp.bfloat16)

    def place(chunk, _):
        for off in range(1, sections):
            piece(chunk * (sections - 1) + off - 1, True).wait_recv()
        start = pl.multiple_of(chunk * CHUNK_ROWS, CHUNK_ROWS)
        for old in range(ROW_BLOCKS):
            first = old % per_section * block_rows
            moved[old] = held[
                old // per_section, pl.ds(start, CHUNK_ROWS), first : first + block_rows
            ]
        for block in range(ROW_BLOCKS):
            new_out[0, 0, pl.ds(start, CHUNK_ROWS), block * block_rows : (block + 1) * block_rows] = (
                moved[places[block]]
            )

    lax.fori_loop(0, chunk_count, place, None)

    for outgoing in sent:
        outgoing.wait_send()
    lax.fori_loop(0, piece_count, lambda index, _: piece(index, False).wait_send(), None)


def written(mixed, new_weight):
    rows = new_weight.shape[2] // WRITES

    def kernel(mixed_ref, new_ref, mixed_out, new_out, sems):
        copies = [pltpu.make_async_copy(mixed_ref, mixed_out, sems.at[WRITES])]
        for index in range(WRITES):
            part = (0, 0, pl.ds(index * rows, rows))
            copies.append(
                pltpu.make_async_copy(new_ref.at[part], new_out.at[part], sems.at[index])
            )
        for copy in copies:
            copy.start()
        for copy in copies:
            copy.wait()

    return pl.pallas_call(
        kernel,
        out_shape=(
            jax.ShapeDtypeStruct(mixed.shape, mixed.dtype),
            jax.ShapeDtypeStruct(new_weight.shape, new_weight.dtype),
        ),
        in_specs=[pl.BlockSpec(memory_space=pltpu.VMEM)] * 2,
        out_specs=(pl.BlockSpec(memory_space=pltpu.HBM), pl.BlockSpec(memory_space=pltpu.HBM)),
        scratch_shapes=[pltpu.SemaphoreType.DMA((WRITES + 1,))],
        compiler_params=pltpu.CompilerParams(vmem_limit_bytes=2**20),
    )(
        pltpu.with_memory_space_constraint(mixed, pltpu.VMEM),
        pltpu.with_memory_space_constraint(new_weight, pltpu.VMEM),
    )


def shards(hidden_in, norm_gain, wqkv_old, wo, key_cache, value_cache, lengths, section_order):
    sections = lax.axis_size("tp") // PER_SECTION_TP
    members = PER_SECTION_TP * lax.axis_size("sub")
    seqs, width = hidden_in.shape
    unit_count, rows_old = wqkv_old.shape[2:]
    cols_dev = unit_count // sections
    block_rows = width // ROW_BLOCKS
    positions = key_cache.shape[1]
    own_heads = wo.shape[0] // HEAD_DIM
    head_rows = own_heads * seqs
    share = width // members
    pieces = cols_dev // CHUNK_ROWS * (sections - 1)
    f32, bf16 = jnp.float32, jnp.bfloat16
    heads = HEADS + 2 * KV_HEADS

    def kernel(*refs):
        layer_kernel(sections, *refs)

    scratch = [
        pltpu.VMEM(hidden_in.shape, bf16),
        pltpu.VMEM((1, width), f32),
        pltpu.VMEM((unit_count, rows_old), bf16),
        pltpu.VMEM((sections, cols_dev, rows_old), bf16),
        pltpu.VMEM(wo.shape, bf16),
        pltpu.VMEM(key_cache.shape, bf16),
        pltpu.VMEM(value_cache.shape, bf16),
        pltpu.SMEM(lengths.shape, jnp.int32),
        pltpu.SMEM(section_order.shape, jnp.int32),
        pltpu.SMEM(section_order.shape, jnp.int32),
        pltpu.VMEM((ROW_BLOCKS, seqs, block_rows), f32),
        pltpu.VMEM((seqs, rows_old), f32),
        pltpu.VMEM((sections, seqs, unit_count), f32),
        pltpu.VMEM((members, seqs, unit_count), f32),
        pltpu.VMEM((heads * seqs, HEAD_DIM), f32),
        pltpu.VMEM((heads * seqs, HEAD_DIM), f32),
        pltpu.VMEM((sections * members, head_rows, HEAD_DIM), f32),
        pltpu.VMEM((KV_HEADS, head_rows, HEAD_DIM), f32),
        pltpu.VMEM((KV_HEADS, head_rows, HEAD_DIM), f32),
        pltpu.VMEM((HEADS // KV_HEADS * seqs, seqs * positions), f32),
        pltpu.VMEM((HEADS // KV_HEADS * seqs, 2 * HEAD_DIM), f32),
        pltpu.VMEM((members, sections, head_rows, 2 * HEAD_DIM), f32),
        pltpu.VMEM((members, sections, head_rows, 2 * HEAD_DIM), f32),
        pltpu.VMEM((sections, head_rows, 2 * HEAD_DIM), f32),
        pltpu.VMEM((sections, head_rows, 2 * HEAD_DIM), f32),
        pltpu.VMEM((head_rows, HEAD_DIM), f32),
        pltpu.VMEM((members, seqs, share), f32),
        pltpu.VMEM((members, seqs, share), f32),
        pltpu.VMEM((sections, seqs, share), f32),
        pltpu.VMEM((members, seqs, share), f32),
        pltpu.VMEM((ROW_BLOCKS, CHUNK_ROWS, block_rows), bf16),
        pltpu.SemaphoreType.DMA((9,)),
        pltpu.SemaphoreType.DMA((pieces,)),
        pltpu.SemaphoreType.DMA((pieces,)),
        pltpu.SemaphoreType.DMA((3, sections - 1)),
        pltpu.SemaphoreType.DMA((3, sections - 1)),
        pltpu.SemaphoreType.DMA((4, members - 1)),
        pltpu.SemaphoreType.DMA((4, members - 1)),
        pltpu.SemaphoreType.REGULAR,
    ]
    with jax.named_scope("layer"):
        results = pl.pallas_call(
            kernel,
            out_shape=(
                pltpu.VMEM((seqs, width), bf16),
                pltpu.VMEM((1, 1, cols_dev, width), bf16),
            ),
            in_specs=[pl.BlockSpec(memory_space=pltpu.HBM)] * 8,
            out_specs=(pl.BlockSpec(memory_space=pltpu.VMEM), pl.BlockSpec(memory_space=pltpu.VMEM)),
            scratch_shapes=scratch,
            compiler_params=pltpu.CompilerParams(
                collective_id=0, has_side_effects=True, vmem_limit_bytes=45 * 2**20
            ),
        )(
            hidden_in,
            norm_gain.reshape(1, width),
            wqkv_old,
            wo,
            key_cache,
            value_cache,
            lengths,
            section_order,
        )
    with jax.named_scope("written"):
        return written(*results)


def solution(mesh):
    placed = (
        P("replica", None),
        P("replica"),
        P(("replica", "tp"), "sub", None, None),
        P(("replica", "tp", "sub"), None),
        P("replica", ("tp", "sub"), None),
        P("replica", ("tp", "sub"), None),
        P("replica"),
        P("replica"),
    )
    return jax.shard_map(
        shards,
        mesh=mesh,
        in_specs=placed,
        out_specs=(P("replica", None), P(("replica", "tp"), "sub", None, None)),
        check_vma=False,
    )
```

```python
import math

import jax
import jax.numpy as jnp
from jax import lax
from jax.experimental import pallas as pl
from jax.experimental.pallas import tpu as pltpu
from jax.sharding import PartitionSpec as P

HEADS = 64
KV_HEADS = 8
HEAD_DIM = 128
RANKS = 8
ROW_BLOCKS = 16
PER_SECTION_TP = 4
CHUNK_ROWS = 16
AHEAD = 4
EARLY_TENTHS = 7
LEAD = 2
HOLD = 4
TRIGGER = 1
MESH = pl.DeviceIdType.MESH
CONTRACT_LAST = (((1,), (1,)), ((), ()))


def early_count(chunk_count):
    return max(1, chunk_count * EARLY_TENTHS // 10)


def layer_kernel(
    sections,
    hidden_in,
    gain_in,
    w_in,
    wo_in,
    key_in,
    value_in,
    lengths_in,
    order_in,
    mixed_out,
    new_out,
    hidden,
    gain,
    weight,
    held,
    wo,
    keys,
    values,
    lengths,
    order,
    places,
    normed,
    own_rows,
    x1,
    units,
    raw,
    turned,
    own_q,
    new_k,
    new_v,
    mask,
    mixes,
    parts,
    x2,
    merged,
    x3,
    attended,
    shares,
    x4,
    x5,
    x6,
    moved,
    load_sems,
    bulk_send,
    bulk_recv,
    cross_send,
    cross_recv,
    side_send,
    side_recv,
    section_in,
):
    members = RANKS
    replica = lax.axis_index("replica")
    tp = lax.axis_index("tp")
    sub = lax.axis_index("sub")
    section = tp // PER_SECTION_TP
    column = lax.rem(tp, PER_SECTION_TP)
    member = column * 2 + sub
    rank = section * members + member

    seqs, width = hidden.shape
    cols_dev = held.shape[1]
    rows_old = held.shape[2]
    per_section = ROW_BLOCKS // sections
    block_rows = rows_old // per_section
    unit_count = weight.shape[0]
    positions = keys.shape[1]
    own_heads = own_q.shape[1] // seqs
    head_rows = own_heads * seqs
    chunk_count = cols_dev // CHUNK_ROWS
    early_chunks = early_count(chunk_count)
    late = column >= PER_SECTION_TP // 2
    chunks_here = jnp.where(late, early_chunks, chunk_count)
    early_pieces = early_chunks * (sections - 1)
    piece_count = chunk_count * (sections - 1)
    inverse = 1.0 / math.sqrt(HEAD_DIM)
    groups = HEADS // KV_HEADS
    share = width // members

    def cross_peer(off):
        other = lax.rem(section + off, sections)
        return other, (replica, other * PER_SECTION_TP + column, sub)

    def side_peer(off):
        other = lax.rem(member + off, members)
        return other, (replica, section * PER_SECTION_TP + other // 2, lax.rem(other, 2))

    barrier = pltpu.get_barrier_semaphore()
    is_first = member == 0
    for off in range(1, sections):
        pl.semaphore_signal(barrier, inc=1, device_id=cross_peer(off)[1], device_id_type=MESH)

    @pl.when(jnp.logical_not(is_first))
    def _():
        pl.semaphore_signal(
            barrier,
            inc=1,
            device_id=(replica, section * PER_SECTION_TP, 0),
            device_id_type=MESH,
        )

    own_start = pl.multiple_of(section * cols_dev, CHUNK_ROWS)
    loads = [
        pltpu.make_async_copy(source, target, load_sems.at[index])
        for index, (source, target) in enumerate(
            (
                (hidden_in, hidden),
                (gain_in, gain),
                (order_in, order),
                (lengths_in, lengths),
                (w_in.at[0, 0], weight),
                (key_in, keys),
                (value_in, values),
                (wo_in, wo),
                (w_in.at[0, 0, pl.ds(own_start, cols_dev)], held.at[section]),
            )
        )
    ]
    for load in loads:
        load.start()
    pl.semaphore_wait(barrier, sections - 1 + jnp.where(is_first, members - 1, 0))

    @pl.when(is_first)
    def _():
        for off in range(1, members):
            pl.semaphore_signal(
                section_in, inc=1, device_id=side_peer(off)[1], device_id_type=MESH
            )

    def piece(index, arriving):
        chunk = index // (sections - 1)
        off = lax.rem(index, sections - 1) + 1
        other, peer = cross_peer(off)
        start = pl.multiple_of(chunk * CHUNK_ROWS, CHUNK_ROWS)
        slot = lax.rem(section + sections - off, sections) if arriving else section
        return pltpu.make_async_remote_copy(
            src_ref=w_in.at[
                0, 0, pl.ds(pl.multiple_of(other * cols_dev + start, CHUNK_ROWS), CHUNK_ROWS)
            ],
            dst_ref=held.at[slot, pl.ds(start, CHUNK_ROWS)],
            send_sem=bulk_send.at[index],
            recv_sem=bulk_recv.at[index],
            device_id=peer,
            device_id_type=MESH,
        )

    queued = [0]

    def queue(count):
        first = queued[0]
        last = min(first + count, early_pieces)
        queued[0] = last
        if last > first:
            lax.fori_loop(first, last, lambda index, _: piece(index, False).start(), None)

    sent = []

    def cross_swap(step, source_of, target):
        def copy(off, arriving):
            other, peer = cross_peer(off)
            slot = lax.rem(section + sections - off, sections) if arriving else section
            return pltpu.make_async_remote_copy(
                src_ref=source_of(other),
                dst_ref=target.at[slot],
                send_sem=cross_send.at[step, off - 1],
                recv_sem=cross_recv.at[step, off - 1],
                device_id=peer,
                device_id_type=MESH,
            )

        for off in range(1, sections):
            outgoing = copy(off, False)
            outgoing.start()
            sent.append(outgoing)
        return lambda: [copy(off, True).wait_recv() for off in range(1, sections)]

    def side_swap(step, source_of, target):
        def copy(off, arriving):
            other, peer = side_peer(off)
            slot = lax.rem(member + members - off, members) if arriving else member
            return pltpu.make_async_remote_copy(
                src_ref=source_of(other),
                dst_ref=target.at[slot],
                send_sem=side_send.at[step, off - 1],
                recv_sem=side_recv.at[step, off - 1],
                device_id=peer,
                device_id_type=MESH,
            )

        for off in range(1, members):
            outgoing = copy(off, False)
            outgoing.start()
            sent.append(outgoing)
        return lambda: [copy(off, True).wait_recv() for off in range(1, members)]

    queue(AHEAD)

    for load in loads[:4]:
        load.wait()
    widened = hidden[...].astype(jnp.float32)
    factor = lax.rsqrt(jnp.mean(widened * widened, -1, keepdims=True) + 1e-05)
    rounded = (widened * factor * gain[...]).astype(jnp.bfloat16).astype(jnp.float32)
    for block in range(ROW_BLOCKS):
        normed[block] = rounded[:, block * block_rows : (block + 1) * block_rows]
    for slot in range(per_section):
        own_rows[:, slot * block_rows : (slot + 1) * block_rows] = normed[
            order[section * per_section + slot]
        ]
    loads[4].wait()
    rows = own_rows[...].astype(jnp.bfloat16)
    tile = 256

    def project(step, _):
        start = pl.multiple_of(step * tile, tile)
        x1[section, :, pl.ds(start, tile)] = lax.dot_general(
            rows, weight[pl.ds(start, tile), :], CONTRACT_LAST, preferred_element_type=jnp.float32
        )

    lax.fori_loop(0, unit_count // tile, project, None)
    arrive = cross_swap(0, lambda other: x1.at[section], x1)
    queue(AHEAD)

    row_index = lax.broadcasted_iota(jnp.int32, (8, HEAD_DIM), 0)
    lane_index = lax.broadcasted_iota(jnp.int32, (8, HEAD_DIM), 1)

    def by_seq(seq_of_row):
        picked = jnp.full(seq_of_row.shape, lengths[0], jnp.int32)
        for seq in range(1, seqs):
            picked = jnp.where(seq_of_row == seq, lengths[seq], picked)
        return picked

    half = HEAD_DIM // 2
    pair = jnp.where(lane_index < half, lane_index, lane_index - half).astype(jnp.float32)
    freqs = jnp.exp(pair * (-2.0 * math.log(500000.0) / HEAD_DIM))
    angles = by_seq(lax.rem(row_index, seqs)).astype(jnp.float32) * freqs
    cosine = jnp.cos(angles)
    sine = jnp.where(lane_index < half, -jnp.sin(angles), jnp.sin(angles))

    wide = (groups * seqs, seqs * positions)
    seq_of_row = lax.rem(lax.broadcasted_iota(jnp.int32, wide, 0), seqs)
    at = lax.broadcasted_iota(jnp.int32, wide, 1)
    usable = (at // positions == seq_of_row) & (
        rank * positions + lax.rem(at, positions) < by_seq(seq_of_row)
    )
    mask[...] = jnp.where(usable, 1.0, 0.0)

    def find(block, _):
        place = jnp.int32(0)
        for old in range(ROW_BLOCKS):
            place = jnp.where(order[old] == block, old, place)
        places[block] = place

    lax.fori_loop(0, ROW_BLOCKS, find, None)

    arrive()
    total = x1[0]
    for other in range(1, sections):
        total = total + x1[other]
    units[member] = total.astype(jnp.bfloat16).astype(jnp.float32)

    @pl.when(jnp.logical_not(is_first))
    def _():
        pl.semaphore_wait(section_in, 1)

    arrive = side_swap(0, lambda other: units.at[member], units)
    queue(AHEAD)
    for load in loads[5:]:
        load.wait()
    arrive()

    per_rank = unit_count // HEAD_DIM
    for head in range(HEADS + 2 * KV_HEADS):
        lane = (head % per_rank) * HEAD_DIM
        raw[head * seqs : (head + 1) * seqs, :] = units[
            head // per_rank, :, lane : lane + HEAD_DIM
        ]

    def turn(step, _):
        start = pl.multiple_of(step * 8, 8)
        vectors = raw[pl.ds(start, 8), :]
        out = vectors * cosine + pltpu.roll(vectors, half, 1) * sine
        turned[pl.ds(start, 8), :] = out.astype(jnp.bfloat16).astype(jnp.float32)

    lax.fori_loop(0, (HEADS + KV_HEADS) * seqs // 8, turn, None)
    for owner in range(sections * members):
        own_q[owner] = turned[owner * head_rows : (owner + 1) * head_rows, :]
    for head in range(KV_HEADS):
        key_row = (HEADS + head) * seqs
        value_row = (HEADS + KV_HEADS + head) * seqs
        for copy in range(own_heads):
            new_k[head, copy * seqs : (copy + 1) * seqs, :] = turned[key_row : key_row + seqs, :]
            new_v[head, copy * seqs : (copy + 1) * seqs, :] = raw[value_row : value_row + seqs, :]

    owners = groups // own_heads
    stat_lane = lax.broadcasted_iota(jnp.int32, (groups * seqs, HEAD_DIM), 1)

    def attend(head, _):
        lane = pl.ds(pl.multiple_of(head * HEAD_DIM, HEAD_DIM), HEAD_DIM)
        row = pl.multiple_of(head * groups * seqs, groups * seqs)
        query = turned[pl.ds(row, groups * seqs), :].astype(jnp.bfloat16)
        key = keys[:, :, lane].reshape(seqs * positions, HEAD_DIM)
        value = values[:, :, lane].reshape(seqs * positions, HEAD_DIM)
        open_ = mask[...] > 0.5
        scores = (
            lax.dot_general(query, key, CONTRACT_LAST, preferred_element_type=jnp.float32)
            * inverse
        )
        top = jnp.max(jnp.where(open_, scores, -1e30), -1, keepdims=True)
        weights = jnp.exp(jnp.where(open_, scores - top, -1e30))
        summed = jnp.sum(weights, -1, keepdims=True)
        high = weights.astype(jnp.bfloat16)
        low = (weights - high.astype(jnp.float32)).astype(jnp.bfloat16)
        mixes[:, :HEAD_DIM] = jnp.dot(
            high, value, preferred_element_type=jnp.float32
        ) + jnp.dot(low, value, preferred_element_type=jnp.float32)
        mixes[:, HEAD_DIM:] = jnp.where(stat_lane < half, top, summed)
        for index in range(owners):
            owner = head * owners + index
            parts[lax.rem(owner, members), owner // members] = mixes[
                index * head_rows : (index + 1) * head_rows, :
            ]

    lax.fori_loop(0, KV_HEADS, attend, None)
    arrive = side_swap(1, lambda other: parts.at[other], x2)
    x2[member] = parts[member]
    queue(AHEAD)
    arrive()

    def combined(refs):
        best = refs[0][:, HEAD_DIM : HEAD_DIM + 1]
        for ref in refs[1:]:
            best = jnp.maximum(best, ref[:, HEAD_DIM : HEAD_DIM + 1])
        mix = jnp.zeros((head_rows, HEAD_DIM), jnp.float32)
        summed = jnp.zeros((head_rows, 1), jnp.float32)
        for ref in refs:
            scale = jnp.exp(ref[:, HEAD_DIM : HEAD_DIM + 1] - best)
            mix = mix + ref[:, :HEAD_DIM] * scale
            summed = summed + ref[:, HEAD_DIM + half : HEAD_DIM + half + 1] * scale
        return best, summed, mix

    own_lane = lax.broadcasted_iota(jnp.int32, (head_rows, HEAD_DIM), 1)
    for other in range(sections):
        best, summed, mix = combined([x2[source, other] for source in range(members)])
        merged[other, :, :HEAD_DIM] = mix
        merged[other, :, HEAD_DIM:] = jnp.where(own_lane < half, best, summed)
    arrive = cross_swap(1, lambda other: merged.at[other], x3)
    x3[section] = merged[section]
    queue(AHEAD)
    arrive()

    best, summed, mix = combined([x3[source] for source in range(sections)])
    kv_head = rank * own_heads // groups
    own_score = jnp.sum(own_q[rank] * new_k[kv_head], -1, keepdims=True) * inverse
    highest = jnp.maximum(best, own_score)
    old_scale = jnp.exp(best - highest)
    own_weight = jnp.exp(own_score - highest)
    numerator = mix * old_scale + own_weight * new_v[kv_head]
    denominator = summed * old_scale + own_weight
    attended[...] = numerator / denominator
    flat = jnp.concatenate(
        [attended[head * seqs : (head + 1) * seqs, :] for head in range(own_heads)], -1
    ).astype(jnp.bfloat16)

    def give(other, _):
        lane = pl.ds(pl.multiple_of(other * share, share), share)
        shares[other] = jnp.dot(flat, wo[:, lane], preferred_element_type=jnp.float32)

    lax.fori_loop(0, members, give, None)
    arrive = side_swap(2, lambda other: shares.at[other], x4)
    x4[member] = shares[member]
    queue(AHEAD)
    arrive()

    total = x4[0]
    for other in range(1, members):
        total = total + x4[other]
    x5[section] = total
    arrive = cross_swap(2, lambda other: x5.at[section], x5)
    queue(AHEAD)
    arrive()

    total = hidden[:, pl.ds(pl.multiple_of(member * share, share), share)].astype(jnp.float32)
    product = x5[0]
    for other in range(1, sections):
        product = product + x5[other]
    x6[member] = (total + product).astype(jnp.bfloat16).astype(jnp.float32)
    arrive = side_swap(3, lambda other: x6.at[member], x6)
    queue(early_pieces)

    hold = min(HOLD, chunk_count - early_chunks)
    free_pieces = (chunk_count - hold) * (sections - 1)
    holds = jnp.logical_not(late) & (section == 0)

    @pl.when(jnp.logical_not(late))
    def _():
        lax.fori_loop(
            early_pieces,
            jnp.where(holds, free_pieces, piece_count),
            lambda index, _: piece(index, False).start(),
            None,
        )

    arrive()
    for other in range(members):
        mixed_out[:, other * share : (other + 1) * share] = x6[other].astype(jnp.bfloat16)

    def place(chunk, _):
        for off in range(1, sections):
            piece(chunk * (sections - 1) + off - 1, True).wait_recv()

        @pl.when(holds & (chunk == chunk_count - hold - TRIGGER))
        def _():
            lax.fori_loop(
                free_pieces, piece_count, lambda index, _: piece(index, False).start(), None
            )

        start = pl.multiple_of(chunk * CHUNK_ROWS, CHUNK_ROWS)
        for old in range(ROW_BLOCKS):
            first = old % per_section * block_rows
            moved[old] = held[
                old // per_section, pl.ds(start, CHUNK_ROWS), first : first + block_rows
            ]
        for block in range(ROW_BLOCKS):
            new_out[0, 0, pl.ds(start, CHUNK_ROWS), block * block_rows : (block + 1) * block_rows] = (
                moved[places[block]]
            )

    lax.fori_loop(0, chunks_here, place, None)

    for outgoing in sent:
        outgoing.wait_send()
    lax.fori_loop(
        0,
        chunks_here * (sections - 1),
        lambda index, _: piece(index, False).wait_send(),
        None,
    )


def rest_kernel(
    sections,
    early_chunks,
    w_in,
    order_in,
    written_in,
    new_out,
    held,
    order,
    places,
    moved,
    load_sems,
    bulk_send,
    bulk_recv,
):
    replica = lax.axis_index("replica")
    tp = lax.axis_index("tp")
    sub = lax.axis_index("sub")
    section = tp // PER_SECTION_TP
    column = lax.rem(tp, PER_SECTION_TP)
    rows_here, rows_old = held.shape[1:]
    cols_dev = early_chunks * CHUNK_ROWS + rows_here
    per_section = ROW_BLOCKS // sections
    block_rows = rows_old // per_section
    chunk_count = rows_here // CHUNK_ROWS
    piece_count = chunk_count * (sections - 1)

    def cross_peer(off):
        other = lax.rem(section + off, sections)
        return other, (replica, other * PER_SECTION_TP + column, sub)

    def piece(index, arriving):
        chunk = index // (sections - 1)
        off = lax.rem(index, sections - 1) + 1
        other, peer = cross_peer(off)
        start = pl.multiple_of(chunk * CHUNK_ROWS, CHUNK_ROWS)
        source = pl.multiple_of(
            other * cols_dev + early_chunks * CHUNK_ROWS + start, CHUNK_ROWS
        )
        slot = lax.rem(section + sections - off, sections) if arriving else section
        return pltpu.make_async_remote_copy(
            src_ref=w_in.at[0, 0, pl.ds(source, CHUNK_ROWS)],
            dst_ref=held.at[slot, pl.ds(start, CHUNK_ROWS)],
            send_sem=bulk_send.at[index],
            recv_sem=bulk_recv.at[index],
            device_id=peer,
            device_id_type=MESH,
        )

    def send(first, last):
        lax.fori_loop(first, last, lambda index, _: piece(index, False).start(), None)

    paced = section == sections - 1
    lead = min(LEAD, chunk_count)

    @pl.when(column >= PER_SECTION_TP // 2)
    def _():
        barrier = pltpu.get_barrier_semaphore()
        for off in range(1, sections):
            pl.semaphore_signal(barrier, inc=1, device_id=cross_peer(off)[1], device_id_type=MESH)
        own_start = pl.multiple_of(section * cols_dev + early_chunks * CHUNK_ROWS, CHUNK_ROWS)
        loads = [
            pltpu.make_async_copy(order_in, order, load_sems.at[0]),
            pltpu.make_async_copy(
                w_in.at[0, 0, pl.ds(own_start, rows_here)], held.at[section], load_sems.at[1]
            ),
        ]
        for load in loads:
            load.start()
        pl.semaphore_wait(barrier, sections - 1)
        send(0, lead * (sections - 1))

        @pl.when(jnp.logical_not(paced))
        def _():
            send(lead * (sections - 1), piece_count)

        for load in loads:
            load.wait()

        def find(block, _):
            place = jnp.int32(0)
            for old in range(ROW_BLOCKS):
                place = jnp.where(order[old] == block, old, place)
            places[block] = place

        lax.fori_loop(0, ROW_BLOCKS, find, None)

        def place(chunk, _):
            for off in range(1, sections):
                piece(chunk * (sections - 1) + off - 1, True).wait_recv()

            @pl.when(paced & (chunk + lead < chunk_count))
            def _():
                send((chunk + lead) * (sections - 1), (chunk + lead + 1) * (sections - 1))

            start = pl.multiple_of(chunk * CHUNK_ROWS, CHUNK_ROWS)
            for old in range(ROW_BLOCKS):
                first = old % per_section * block_rows
                moved[old] = held[
                    old // per_section, pl.ds(start, CHUNK_ROWS), first : first + block_rows
                ]
            for block in range(ROW_BLOCKS):
                new_out[
                    0, 0, pl.ds(start, CHUNK_ROWS), block * block_rows : (block + 1) * block_rows
                ] = moved[places[block]]

        lax.fori_loop(0, chunk_count, place, None)
        lax.fori_loop(0, piece_count, lambda index, _: piece(index, False).wait_send(), None)


def written(mixed, new_weight):
    cols_dev = new_weight.shape[2]
    early_rows = early_count(cols_dev // CHUNK_ROWS) * CHUNK_ROWS

    def kernel(mixed_ref, new_ref, mixed_out, new_out, sems):
        def copy(first, rows, index):
            part = (0, 0, pl.ds(first, rows))
            return pltpu.make_async_copy(new_ref.at[part], new_out.at[part], sems.at[index])

        all_rows = lax.rem(lax.axis_index("tp"), PER_SECTION_TP) < PER_SECTION_TP // 2
        copies = [
            copy(0, early_rows, 0),
            pltpu.make_async_copy(mixed_ref, mixed_out, sems.at[1]),
        ]
        for each in copies:
            each.start()

        @pl.when(all_rows)
        def _():
            late = copy(early_rows, cols_dev - early_rows, 2)
            late.start()
            late.wait()

        for each in copies:
            each.wait()

    return pl.pallas_call(
        kernel,
        out_shape=(
            jax.ShapeDtypeStruct(mixed.shape, mixed.dtype),
            jax.ShapeDtypeStruct(new_weight.shape, new_weight.dtype),
        ),
        in_specs=[pl.BlockSpec(memory_space=pltpu.VMEM)] * 2,
        out_specs=(pl.BlockSpec(memory_space=pltpu.HBM), pl.BlockSpec(memory_space=pltpu.HBM)),
        scratch_shapes=[pltpu.SemaphoreType.DMA((3,))],
        compiler_params=pltpu.CompilerParams(vmem_limit_bytes=2**20),
    )(
        pltpu.with_memory_space_constraint(mixed, pltpu.VMEM),
        pltpu.with_memory_space_constraint(new_weight, pltpu.VMEM),
    )


def finished(new_weight, rest):
    rows = rest.shape[2]
    first = new_weight.shape[2] - rows

    def kernel(new_ref, rest_ref, new_out, sem):
        @pl.when(lax.rem(lax.axis_index("tp"), PER_SECTION_TP) >= PER_SECTION_TP // 2)
        def _():
            copy = pltpu.make_async_copy(rest_ref, new_out.at[:, :, pl.ds(first, rows)], sem)
            copy.start()
            copy.wait()

    return pl.pallas_call(
        kernel,
        out_shape=jax.ShapeDtypeStruct(new_weight.shape, new_weight.dtype),
        in_specs=[
            pl.BlockSpec(memory_space=pltpu.HBM),
            pl.BlockSpec(memory_space=pltpu.VMEM),
        ],
        out_specs=pl.BlockSpec(memory_space=pltpu.HBM),
        scratch_shapes=[pltpu.SemaphoreType.DMA],
        input_output_aliases={0: 0},
        compiler_params=pltpu.CompilerParams(vmem_limit_bytes=2**20),
    )(new_weight, pltpu.with_memory_space_constraint(rest, pltpu.VMEM))


def shards(hidden_in, norm_gain, wqkv_old, wo, key_cache, value_cache, lengths, section_order):
    sections = lax.axis_size("tp") // PER_SECTION_TP
    members = PER_SECTION_TP * lax.axis_size("sub")
    seqs, width = hidden_in.shape
    unit_count, rows_old = wqkv_old.shape[2:]
    cols_dev = unit_count // sections
    block_rows = width // ROW_BLOCKS
    positions = key_cache.shape[1]
    own_heads = wo.shape[0] // HEAD_DIM
    head_rows = own_heads * seqs
    share = width // members
    pieces = cols_dev // CHUNK_ROWS * (sections - 1)
    f32, bf16 = jnp.float32, jnp.bfloat16
    heads = HEADS + 2 * KV_HEADS

    def kernel(*refs):
        layer_kernel(sections, *refs)

    scratch = [
        pltpu.VMEM(hidden_in.shape, bf16),
        pltpu.VMEM((1, width), f32),
        pltpu.VMEM((unit_count, rows_old), bf16),
        pltpu.VMEM((sections, cols_dev, rows_old), bf16),
        pltpu.VMEM(wo.shape, bf16),
        pltpu.VMEM(key_cache.shape, bf16),
        pltpu.VMEM(value_cache.shape, bf16),
        pltpu.SMEM(lengths.shape, jnp.int32),
        pltpu.SMEM(section_order.shape, jnp.int32),
        pltpu.SMEM(section_order.shape, jnp.int32),
        pltpu.VMEM((ROW_BLOCKS, seqs, block_rows), f32),
        pltpu.VMEM((seqs, rows_old), f32),
        pltpu.VMEM((sections, seqs, unit_count), f32),
        pltpu.VMEM((members, seqs, unit_count), f32),
        pltpu.VMEM((heads * seqs, HEAD_DIM), f32),
        pltpu.VMEM((heads * seqs, HEAD_DIM), f32),
        pltpu.VMEM((sections * members, head_rows, HEAD_DIM), f32),
        pltpu.VMEM((KV_HEADS, head_rows, HEAD_DIM), f32),
        pltpu.VMEM((KV_HEADS, head_rows, HEAD_DIM), f32),
        pltpu.VMEM((HEADS // KV_HEADS * seqs, seqs * positions), f32),
        pltpu.VMEM((HEADS // KV_HEADS * seqs, 2 * HEAD_DIM), f32),
        pltpu.VMEM((members, sections, head_rows, 2 * HEAD_DIM), f32),
        pltpu.VMEM((members, sections, head_rows, 2 * HEAD_DIM), f32),
        pltpu.VMEM((sections, head_rows, 2 * HEAD_DIM), f32),
        pltpu.VMEM((sections, head_rows, 2 * HEAD_DIM), f32),
        pltpu.VMEM((head_rows, HEAD_DIM), f32),
        pltpu.VMEM((members, seqs, share), f32),
        pltpu.VMEM((members, seqs, share), f32),
        pltpu.VMEM((sections, seqs, share), f32),
        pltpu.VMEM((members, seqs, share), f32),
        pltpu.VMEM((ROW_BLOCKS, CHUNK_ROWS, block_rows), bf16),
        pltpu.SemaphoreType.DMA((9,)),
        pltpu.SemaphoreType.DMA((pieces,)),
        pltpu.SemaphoreType.DMA((pieces,)),
        pltpu.SemaphoreType.DMA((3, sections - 1)),
        pltpu.SemaphoreType.DMA((3, sections - 1)),
        pltpu.SemaphoreType.DMA((4, members - 1)),
        pltpu.SemaphoreType.DMA((4, members - 1)),
        pltpu.SemaphoreType.REGULAR,
    ]
    with jax.named_scope("layer"):
        results = pl.pallas_call(
            kernel,
            out_shape=(
                pltpu.VMEM((seqs, width), bf16),
                pltpu.VMEM((1, 1, cols_dev, width), bf16),
            ),
            in_specs=[pl.BlockSpec(memory_space=pltpu.HBM)] * 8,
            out_specs=(pl.BlockSpec(memory_space=pltpu.VMEM), pl.BlockSpec(memory_space=pltpu.VMEM)),
            scratch_shapes=scratch,
            compiler_params=pltpu.CompilerParams(
                collective_id=0, has_side_effects=True, vmem_limit_bytes=45 * 2**20
            ),
        )(
            hidden_in,
            norm_gain.reshape(1, width),
            wqkv_old,
            wo,
            key_cache,
            value_cache,
            lengths,
            section_order,
        )
    with jax.named_scope("written"):
        mixed, new_weight = written(*results)
    early_chunks = early_count(cols_dev // CHUNK_ROWS)
    rest_rows = cols_dev - early_chunks * CHUNK_ROWS
    rest_pieces = rest_rows // CHUNK_ROWS * (sections - 1)

    def late_kernel(*refs):
        rest_kernel(sections, early_chunks, *refs)

    with jax.named_scope("rest"):
        rest = pl.pallas_call(
            late_kernel,
            out_shape=pltpu.VMEM((1, 1, rest_rows, width), bf16),
            in_specs=[pl.BlockSpec(memory_space=pltpu.HBM)] * 3,
            out_specs=pl.BlockSpec(memory_space=pltpu.VMEM),
            scratch_shapes=[
                pltpu.VMEM((sections, rest_rows, rows_old), bf16),
                pltpu.SMEM(section_order.shape, jnp.int32),
                pltpu.SMEM(section_order.shape, jnp.int32),
                pltpu.VMEM((ROW_BLOCKS, CHUNK_ROWS, block_rows), bf16),
                pltpu.SemaphoreType.DMA((2,)),
                pltpu.SemaphoreType.DMA((rest_pieces,)),
                pltpu.SemaphoreType.DMA((rest_pieces,)),
            ],
            compiler_params=pltpu.CompilerParams(
                collective_id=1, has_side_effects=True, vmem_limit_bytes=16 * 2**20
            ),
        )(
            pltpu.with_memory_space_constraint(wqkv_old, pltpu.HBM),
            pltpu.with_memory_space_constraint(section_order, pltpu.HBM),
            pltpu.with_memory_space_constraint(mixed, pltpu.HBM),
        )
    with jax.named_scope("finished"):
        return mixed, finished(new_weight, rest)


def solution(mesh):
    placed = (
        P("replica", None),
        P("replica"),
        P(("replica", "tp"), "sub", None, None),
        P(("replica", "tp", "sub"), None),
        P("replica", ("tp", "sub"), None),
        P("replica", ("tp", "sub"), None),
        P("replica"),
        P("replica"),
    )
    return jax.shard_map(
        shards,
        mesh=mesh,
        in_specs=placed,
        out_specs=(P("replica", None), P(("replica", "tp"), "sub", None, None)),
        check_vma=False,
    )
```
